32 devices in a mesh: dp: 8 (over z, y), mp: 4 (over x, core).
Axes of the slice: x: 2, y: 2, z: 4, core: 2. Of those that a mesh axis runs over, the one named last changes fastest.
Arguments:
- image_tokens: bfloat16 [8, 192, 3072], P('dp'), may hold values from -6 to 6
- text_tokens: bfloat16 [8, 64, 3072], P('dp'), may hold values from -6 to 6
- null_prompt: bfloat16 [64, 3072], replicated, may hold values from -6 to 6
- drop_flags: int32 [8], P('dp'), may hold values 0 or 1
- time_index: int32 [8], P('dp'), may hold values from 0 to 31
- modulation: float32 [32, 3, 3072], replicated, may hold values from -3 to 3
- w_up: bfloat16 [3072, 12288], P('dp', 'mp'), may hold values from -0.109375 to 0.109375
- w_down: bfloat16 [12288, 3072], P('mp', 'dp'), may hold values from -0.0546875 to 0.0546875
- d_output: bfloat16 [8, 256, 3072], P('dp'), may hold values from -6 to 6
Outputs:
- block_out: bfloat16 [8, 256, 3072], P('dp')
- d_tokens: bfloat16 [8, 256, 3072], P('dp')
- grad_up: float32 [3072, 12288], P('dp', 'mp')
- grad_down: float32 [12288, 3072], P('mp', 'dp')
- grad_null: float32 [64, 3072], replicated
The draws below stay inside these ranges and needn't reach their ends.
All inputs are finite; a program needn't handle non-finite values. No bound on the sum of `drop_flags` on one device may be relied on, other than what follows from the above.
Results may differ from the reference program's by a relative error of at most 0.017.
Values may be sent and summed in bfloat16 or wider, within the bound.
A program may use at most 128 MiB of HBM per device.

```python
import jax
import jax.numpy as jnp
from jax import lax

D = 3072
FF = 12288
L_IMG = 192
L_TXT = 64
NT = 32
B = 8
L = 256
N_MP = 4


def touch_ends(values, stream_key, low, largest):
    extent = values.shape
    place = [jax.random.randint(jax.random.fold_in(stream_key, axis), (), 0, extent[axis]) for axis in range(len(extent))]
    values = values.at[tuple(place)].set(low)
    longest = extent.index(max(extent))
    place[longest] = (place[longest] + 1) % extent[longest]
    return values.at[tuple(place)].set(largest)


def block_levels(key, shape, pieces, low, largest):
    gain = 1.0
    for axis_at, shards_of in pieces:
        heights = jax.random.uniform(jax.random.fold_in(jax.random.fold_in(key, 6), axis_at), (shards_of,), jnp.float32, low / len(pieces), largest / len(pieces))
        gain = gain * jnp.repeat(jnp.exp(heights), shape[axis_at] // shards_of).reshape((-1,) + (1,) * (len(shape) - 1 - axis_at))
    return gain


def gaussian(rng, dims, scale, most, shards=(), held_as=jnp.bfloat16):
    result = jax.random.normal(rng, dims, jnp.float32) * scale
    if len(shards) > 0:
        result = block_levels(rng, dims, shards, -0.22, 0.18) * result
    return jnp.clip(result, min=-most, max=most).astype(held_as)


def setup_inputs(seed: int = 0) -> dict:
    key_list = jax.random.split(jax.random.key(seed), 10)
    return {
        "image_tokens": gaussian(key_list[0], (B, L_IMG, D), 1.0, 6.0, ((0, 8),)),
        "text_tokens": gaussian(key_list[1], (B, L_TXT, D), 1.0, 6.0, ((0, 8),)),
        "null_prompt": gaussian(key_list[2], (L_TXT, D), 1.0, 6.0),
        "drop_flags": touch_ends((jax.random.randint(key_list[3], (B,), 0, 2) < 1).astype(jnp.int32), jax.random.fold_in(key_list[3], 1), 0, 1),
        "time_index": touch_ends(jax.random.randint(key_list[4], (B,), 0, NT), jax.random.fold_in(key_list[4], 1), 0, NT - 1).astype(jnp.int32),
        "modulation": gaussian(key_list[5], (NT, 3, D), 0.5, 3.0, (), jnp.float32),
        "w_up": gaussian(key_list[6], (D, FF), D ** -0.5, 0.109375, ((0, 8), (1, 4))),
        "w_down": gaussian(key_list[7], (FF, D), FF ** -0.5, 0.0546875, ((0, 4), (1, 8))),
        "d_output": gaussian(key_list[8], (B, L, D), 1.0, 6.0, ((0, 8),)),
    }


EPS = 1e-06

def gelu_tanh(values):
    return jax.nn.gelu(values, approximate=True)

def reference(image_tokens, text_tokens, null_prompt, drop_flags, time_index, modulation, w_up, w_down, d_output):
    dropped = drop_flags == 1
    text_in = jnp.where(dropped[:, None, None], null_prompt[None], text_tokens)
    joined = jnp.concatenate([text_in, image_tokens], axis=1)
    levels = jnp.arange(modulation.shape[0], dtype=jnp.int32)
    indicator_matrix = (time_index[:, None] == levels[None, :]).astype(jnp.float32)
    modulation_vectors = jnp.einsum('yi,imr->ymr', indicator_matrix, modulation.astype(jnp.float32), precision=lax.Precision.HIGHEST)
    shift_modulation = modulation_vectors[:, 0][:, None]
    scale_mod = modulation_vectors[:, 1][:, None]
    gate_mod = modulation_vectors[:, 2][:, None]
    batch, length, width = joined.shape
    joined32 = joined.astype(jnp.float32)
    centred = joined32 - lax.optimization_barrier(jnp.mean(joined32, axis=-1, keepdims=True))
    inv_std = lax.rsqrt(lax.optimization_barrier(jnp.mean(centred * centred, axis=-1, keepdims=True)) + EPS)
    normed = centred * inv_std
    mod_in = (normed * (1.0 + scale_mod) + shift_modulation).astype(jnp.bfloat16)
    flat_in = mod_in.reshape(batch * length, width)
    preactivation_rows = jnp.dot(flat_in, w_up, preferred_element_type=jnp.float32)
    hidden = gelu_tanh(preactivation_rows).astype(jnp.bfloat16)
    per_part = w_up.shape[1] // N_MP
    block_ids = jnp.arange(N_MP, dtype=jnp.int32)

    def add_branch(total, block_no):
        start = (block_no * per_part).astype(jnp.int32)
        cols = lax.dynamic_slice_in_dim(hidden, start, per_part, 1)
        rows_w = lax.dynamic_slice_in_dim(w_down, start, per_part, 0)
        part = jnp.dot(cols, rows_w, preferred_element_type=jnp.float32).astype(jnp.bfloat16)
        part = lax.optimization_barrier(part)
        return (total + part.astype(jnp.float32), None)
    branch, _ = lax.scan(add_branch, jnp.zeros((batch * length, width), jnp.float32), block_ids)
    branch = branch.reshape(batch, length, width)
    block_out = (joined32 + gate_mod * branch).astype(jnp.bfloat16)
    d_out32 = d_output.astype(jnp.float32)
    d_branch = (d_out32 * gate_mod).astype(jnp.bfloat16).reshape(batch * length, width)
    hidden_gradient = jnp.dot(d_branch, w_down.T, preferred_element_type=jnp.float32)
    _, gelu_back = jax.vjp(gelu_tanh, preactivation_rows)
    d_pre = gelu_back(hidden_gradient)[0].astype(jnp.bfloat16)
    grad_down = jnp.dot(hidden.T, d_branch, preferred_element_type=jnp.float32)
    grad_up = jnp.dot(flat_in.T, d_pre, preferred_element_type=jnp.float32)

    def add_input(total, block_no):
        start = (block_no * per_part).astype(jnp.int32)
        cols = lax.dynamic_slice_in_dim(d_pre, start, per_part, 1)
        wcols = lax.dynamic_slice_in_dim(w_up, start, per_part, 1)
        part = jnp.dot(cols, wcols.T, preferred_element_type=jnp.float32).astype(jnp.bfloat16)
        part = lax.optimization_barrier(part)
        return (total + part.astype(jnp.float32), None)
    d_mod, _ = lax.scan(add_input, jnp.zeros((batch * length, width), jnp.float32), block_ids)
    d_normed = d_mod.reshape(batch, length, width) * (1.0 + scale_mod)
    d_full = d_out32 + inv_std * (d_normed - lax.optimization_barrier(jnp.mean(d_normed, axis=-1, keepdims=True)) - normed * lax.optimization_barrier(jnp.mean(d_normed * normed, axis=-1, keepdims=True)))
    grad_null = lax.optimization_barrier(jnp.sum(jnp.where(dropped[:, None, None], d_full[:, :L_TXT], jnp.float32(0.0)), axis=0))
    return (block_out, d_full.astype(jnp.bfloat16), grad_up, grad_down, grad_null)
```

```python
import functools

import jax
import jax.numpy as jnp
from jax import lax
from jax.experimental import pallas as pl
from jax.experimental.pallas import tpu as pltpu
from jax.sharding import PartitionSpec as P

EPS = 1e-06
BF16 = jnp.bfloat16
F32 = jnp.float32
MESH = pl.DeviceIdType.MESH
Y = 2
C = 2


def gelu_tanh(values):
    return jax.nn.gelu(values, approximate=True)


def dot(left, right, dims):
    return lax.dot_general(left, right, (dims, ((), ())), preferred_element_type=F32)


def swap(values, axis, size, bit):
    return lax.ppermute(values, axis, [(i, i ^ bit) for i in range(size)])


def generic(
    dp,
    mp,
    image_tokens,
    text_tokens,
    null_prompt,
    drop_flags,
    time_index,
    modulation,
    w_up,
    w_down,
    d_output,
):
    lines = [list(range(parity, dp, 2)) for parity in range(2)]
    per_line = dp // 2
    bits = []
    bit = 1
    while bit < mp:
        bits.append(bit)
        bit *= 2

    d_rows, ff_m = w_up.shape
    f = ff_m // dp
    width = d_rows * dp

    up_own = lax.all_to_all(
        w_up.reshape(d_rows, dp, f).transpose(1, 0, 2), "dp", 0, 0, tiled=True
    ).reshape(width, f)
    down_own = (
        lax.all_to_all(w_down.reshape(dp, f, d_rows), "dp", 0, 0, tiled=True)
        .transpose(1, 0, 2)
        .reshape(f, width)
    )
    up_other = swap(up_own, "dp", dp, 1)
    down_other = swap(down_own, "dp", dp, 1)

    m = lax.axis_index("mp")
    n_text = text_tokens.shape[1] // mp
    n_image = image_tokens.shape[1] // mp
    all_text = text_tokens.shape[1]

    def share(text_part, image_part):
        t = lax.dynamic_slice_in_dim(text_part, m * n_text, n_text, 0)
        i = lax.dynamic_slice_in_dim(image_part, m * n_image, n_image, 0)
        return jnp.concatenate([t, i], axis=0)

    dropped = drop_flags[0] == 1
    joined32 = share(
        jnp.where(dropped, null_prompt, text_tokens[0]), image_tokens[0]
    ).astype(F32)
    d_out32 = share(d_output[0, :all_text], d_output[0, all_text:]).astype(F32)
    level = lax.dynamic_index_in_dim(modulation, time_index[0], 0, keepdims=False)
    shift, scale, gate = level[0][None], level[1][None], level[2][None]
    centred = joined32 - jnp.mean(joined32, axis=-1, keepdims=True)
    inv_std = lax.rsqrt(jnp.mean(centred * centred, axis=-1, keepdims=True) + EPS)
    normed = centred * inv_std
    mod_in = (normed * (1.0 + scale) + shift).astype(BF16)
    d_branch = (d_out32 * gate).astype(BF16)

    def gather(rows):
        rows = lax.all_gather(rows, "dp", axis=0, tiled=True, axis_index_groups=lines)
        for b in reversed(bits):
            rows = jnp.concatenate([rows, swap(rows, "mp", mp, b)], axis=0)
        return rows

    def scatter(own, other, block_own, block_other, contract):
        def product(rows):
            return dot(own[rows], block_own, contract) + dot(other[rows], block_other, contract)

        half = own.shape[0] // 2
        sent = swap(product(slice(half, None)).astype(BF16), "mp", mp, bits[0])
        total = product(slice(0, half)) + sent.astype(F32)
        for b in bits[1:]:
            half = total.shape[0] // 2
            total = total[:half] + swap(total[half:].astype(BF16), "mp", mp, b).astype(F32)
        parts = lax.all_to_all(
            total.astype(BF16).reshape(per_line, -1, width),
            "dp",
            0,
            0,
            tiled=True,
            axis_index_groups=lines,
        )
        return jnp.sum(parts.astype(F32), axis=0)

    tokens = gather(mod_in)
    d_tok = gather(d_branch)

    def half_block(up, down):
        pre = dot(tokens, up, ((1,), (0,)))
        hid, back = jax.vjp(gelu_tanh, pre)
        d_hid = dot(d_tok, down, ((1,), (1,)))
        return hid.astype(BF16), back(d_hid)[0].astype(BF16)

    hid_own, dpre_own = half_block(up_own, down_own)
    hid_other, dpre_other = half_block(up_other, down_other)
    branch = scatter(hid_own, hid_other, down_own, down_other, ((1,), (0,)))
    d_mod = scatter(dpre_own, dpre_other, up_own, up_other, ((1,), (1,)))

    up_sent = dot(tokens, dpre_other, ((0,), (0,))).astype(BF16)
    down_sent = dot(hid_other, d_tok, ((0,), (0,))).astype(BF16)
    up_back = swap(up_sent, "dp", dp, 1)
    down_back = swap(down_sent, "dp", dp, 1)
    g_up = dot(tokens, dpre_own, ((0,), (0,))) + up_back.astype(F32)
    g_down = dot(hid_own, d_tok, ((0,), (0,))) + down_back.astype(F32)
    grad_up = (
        lax.all_to_all(g_up.astype(BF16).reshape(dp, d_rows, f), "dp", 0, 0, tiled=True)
        .transpose(1, 0, 2)
        .reshape(d_rows, ff_m)
        .astype(F32)
    )
    grad_down = (
        lax.all_to_all(
            g_down.astype(BF16).reshape(f, dp, d_rows).transpose(1, 0, 2),
            "dp",
            0,
            0,
            tiled=True,
        )
        .reshape(ff_m, d_rows)
        .astype(F32)
    )

    block_out = (joined32 + gate * branch).astype(BF16)
    d_normed = d_mod * (1.0 + scale)
    d_full = d_out32 + inv_std * (
        d_normed
        - jnp.mean(d_normed, axis=-1, keepdims=True)
        - normed * jnp.mean(d_normed * normed, axis=-1, keepdims=True)
    )
    null_part = jnp.where(dropped, d_full[:n_text], F32(0.0)).astype(BF16)
    null_sum = lax.psum(null_part, "dp")

    def whole(rows):
        every = lax.all_gather(rows, "mp", axis=0)
        return jnp.concatenate(
            [
                every[:, :n_text].reshape(-1, width),
                every[:, n_text:].reshape(-1, width),
            ],
            axis=0,
        )[None]

    grad_null = lax.all_gather(null_sum, "mp", axis=0, tiled=True).astype(F32)
    return (whole(block_out), whole(d_full.astype(BF16)), grad_up, grad_down, grad_null)


class Place:
    def __init__(self, dp, mp):
        self.Z, self.X = dp // Y, mp // C
        d, m = lax.axis_index("dp"), lax.axis_index("mp")
        self.z, self.y = d // Y, d % Y
        self.x, self.c = m // C, m % C
        self.d, self.m = d, m

    def at_z(self, z):
        return (z * Y + self.y, self.m)

    def at_y(self):
        return (self.z * Y + 1 - self.y, self.m)

    def at_x(self, x):
        return (self.d, x * C + self.c)

    def at_c(self):
        return (self.d, self.x * C + 1 - self.c)

    def z_plus(self, j):
        return lax.rem(self.z + j, self.Z)

    def x_plus(self, j):
        return lax.rem(self.x + j, self.X)

    def meet(self):
        barrier = pltpu.get_barrier_semaphore()
        peers = [self.at_z(self.z_plus(j)) for j in range(1, self.Z)]
        peers += [self.at_x(self.x_plus(j)) for j in range(1, self.X)]
        peers += [self.at_y(), self.at_c()]
        for peer in peers:
            pl.semaphore_signal(barrier, inc=1, device_id=peer, device_id_type=MESH)
        pl.semaphore_wait(barrier, len(peers))


class Copies:
    def __init__(self, sems):
        self.sems, self.used, self.open = sems, 0, []

    def go(self, src, dst, recv, device, when=None):
        sem = self.sems.at[self.used]
        self.used += 1

        source, target, peer = src(), dst(), device()

        def make():
            return pltpu.make_async_remote_copy(
                src_ref=source,
                dst_ref=target,
                send_sem=sem,
                recv_sem=recv,
                device_id=peer,
                device_id_type=MESH,
            )

        def start():
            make().start()

        def finish():
            make().wait_send()

        guard(when, start)
        self.open.append((when, finish))

    def local(self, src, dst, when=None):
        sem = self.sems.at[self.used]
        self.used += 1

        source, target = src(), dst()

        def make():
            return pltpu.make_async_copy(source, target, sem)

        def start():
            make().start()

        def finish():
            make().wait()

        guard(when, start)
        self.open.append((when, finish))

    def finish(self):
        for when, wait in self.open:
            guard(when, wait)
        self.open = []


def guard(when, act):
    if when is None:
        act()
    else:
        pl.when(when)(act)


def landed(place, ref, recv, when=None):
    def act():
        pltpu.make_async_remote_copy(
            src_ref=ref(),
            dst_ref=ref(),
            send_sem=recv,
            recv_sem=recv,
            device_id=place.at_y(),
            device_id_type=MESH,
        ).wait_recv()

    guard(when, act)


def tile(index, size):
    return pl.ds(pl.multiple_of(index * size, size), size)


def arrive(dp, mp, nch, own, w_up, w_down, tok, up, down, send, z_tok, x_tok, c_tok, z_w, y_w):
    p = Place(dp, mp)
    Z, X = p.Z, p.X
    dr = w_up.shape[0]
    fz = w_up.shape[1] // Z
    fch = fz // nch
    p.meet()
    cp = Copies(send)

    def up_src(z, k):
        return w_up.at[:, pl.ds(pl.multiple_of(z * fz + k * fch, fch), fch)]

    def down_src(z, k):
        return w_down.at[pl.ds(pl.multiple_of(z * fz + k * fch, fch), fch), :]

    def up_dst(d, k):
        return up.at[tile(d, dr), pl.ds(k * fch, fch)]

    def down_dst(d, k):
        return down.at[pl.ds(k * fch, fch), tile(d, dr)]

    kinds = ((up_src, up_dst), (down_src, down_dst))

    slots = [(0, p.z, None)]
    for s in range(Z - 1):
        slots.append((1 + 2 * s, p.z - 1 - s, p.z - 1 - s >= 0))
        slots.append((2 + 2 * s, p.z + 1 + s, p.z + 1 + s < Z))

    def block(sample, quarter):
        return tok.at[:, sample, quarter]

    def spread(slot, sample, when):
        source = (lambda: own.at[...]) if slot == 0 else (lambda: block(sample, p.m))
        for j in range(1, X):
            cp.go(source, lambda: block(sample, p.m), x_tok.at[j - 1, slot], lambda j=j: p.at_x(p.x_plus(j)), when)
        cp.go(source, lambda: block(sample, p.m), c_tok.at[0, slot], p.at_c, when)

    def pass_on(s):
        for way in (1, -1):
            sample = p.z - s * way
            inside = (sample >= 0) & (p.z + 1 < Z) if way == 1 else (sample < Z) & (p.z >= 1)
            source = (lambda: own.at[...]) if s == 0 else (lambda sample=sample: block(sample, p.m))
            cp.go(
                source,
                lambda sample=sample: block(sample, p.m),
                z_tok.at[(0 if way == 1 else 1), s],
                lambda way=way: p.at_z(p.z + way),
                inside,
            )

    def z_weights(k):
        for j in (2, 1, 3) if Z == 4 else range(1, Z):
            for kind, (src, dst) in enumerate(kinds):
                cp.go(
                    lambda: src(p.z_plus(j), k),
                    lambda: dst(p.d, k),
                    z_w.at[j - 1, k, kind],
                    lambda: p.at_z(p.z_plus(j)),
                )

    pass_on(0)
    spread(*slots[0])
    for k in range(nch):
        for kind, (src, dst) in enumerate(kinds):
            cp.go(lambda: src(p.z, k), lambda: dst(p.d, k), y_w.at[0, k, kind], p.at_y)
    z_weights(0)
    cp.local(lambda: own.at[...], lambda: block(p.z, p.m))
    for k in range(nch):
        for src, dst in kinds:
            cp.local(lambda: src(p.z, k), lambda: dst(p.d, k))

    for s in range(Z - 1):
        for side in (0, 1):
            slot, sample, valid = slots[1 + 2 * s + side]
            landed(p, lambda: block(sample, p.m), z_tok.at[side, s], valid)
        if s < Z - 2:
            pass_on(s + 1)
        for side in (0, 1):
            spread(*slots[1 + 2 * s + side])
    for k in range(1, nch):
        z_weights(k)

    def forward(k):
        for j in (2, 1, 3) if Z == 4 else range(1, Z):
            d_src = lax.rem(p.z - j + Z, Z) * Y + p.y
            for kind, (_, dst) in enumerate(kinds):
                landed(p, lambda: dst(d_src, k), z_w.at[j - 1, k, kind])
                cp.go(lambda: dst(d_src, k), lambda: dst(d_src, k), y_w.at[j, k, kind], p.at_y)

    forward(0)
    for slot, sample, valid in slots:
        for j in range(1, X):
            quarter = lax.rem(p.x - j + X, X) * C + p.c
            landed(p, lambda: block(sample, quarter), x_tok.at[j - 1, slot], valid)
            cp.go(lambda: block(sample, quarter), lambda: block(sample, quarter), c_tok.at[j, slot], p.at_c, valid)
    for k in range(1, nch):
        forward(k)
    for slot, sample, valid in slots:
        for j in range(X):
            quarter = lax.rem(p.x - j + X, X) * C + 1 - p.c
            landed(p, lambda: block(sample, quarter), c_tok.at[j, slot], valid)
    for k in range(nch):
        for j in range(Z):
            d_src = lax.rem(p.z - j + Z, Z) * Y + 1 - p.y
            for kind, (_, dst) in enumerate(kinds):
                landed(p, lambda: dst(d_src, k), y_w.at[j, k, kind])
    cp.finish()


def add_into(target, other, rows, step):
    def body(i, _):
        at = pl.ds(pl.multiple_of(i * step, step), step)
        target[at, :] = (target[at, :].astype(F32) + other[at, :].astype(F32)).astype(BF16)
        return 0

    lax.fori_loop(0, rows // step, body, 0)


def depart(
    dp,
    mp,
    nch,
    n_text,
    g_up,
    g_down,
    branch,
    d_mod,
    joined,
    d_out,
    levels,
    drop,
    fin_all,
    null_all,
    up_out,
    down_out,
    y_up,
    y_down,
    c_buf,
    x_buf,
    r_buf,
    l_buf,
    fin,
    null,
    null_y,
    null_z,
    send,
    y_g,
    z_g,
    c_s,
    x_s,
    r_s,
    l_s,
    f_x,
    f_c,
    n_y,
    n_z,
    n_x,
    n_c,
):
    p = Place(dp, mp)
    Z, X = p.Z, p.X
    fz = g_up.shape[1]
    fch = fz // nch
    width = g_up.shape[0]
    dr = width // (Z * Y)
    n = joined.shape[0]
    p.meet()
    cp = Copies(send)
    partial = (branch, d_mod)
    order = []
    for i in range((Z + 1) // 2):
        order += [Z - 1 - i] + ([i] if i != Z - 1 - i else [])

    def rows_of(sample, x, c):
        return pl.ds(pl.multiple_of(sample * (X * C * n) + (x * C + c) * n, n), n)

    for t in order:
        for i in range(2):
            for j in range(X):
                x = p.x_plus(j + 1)
                cp.go(
                    lambda: partial[i].at[rows_of(t, x, 1 - p.c), :],
                    lambda: c_buf.at[i, t, x],
                    c_s.at[i, t, j],
                    p.at_c,
                )

    def up_rows(z, y):
        return tile(z * Y + y, dr)

    jorder = [2, 1, 3, 0] if Z == 4 else [j for j in range(1, Z)] + [0]
    pieces = [(k, j, kind) for k in range(nch) for j in jorder for kind in range(2)]

    def g_ref(ref, kind, z, y, k):
        cols = pl.ds(k * fch, fch)
        return ref.at[up_rows(z, y), cols] if kind == 0 else ref.at[cols, up_rows(z, y)]

    def y_ref(kind, z, k):
        cols = pl.ds(k * fch, fch)
        return y_up.at[tile(z, dr), cols] if kind == 0 else y_down.at[cols, tile(z, dr)]

    def out_ref(kind, z, k):
        cols = pl.ds(pl.multiple_of(z * fz + k * fch, fch), fch)
        return up_out.at[:, cols] if kind == 0 else down_out.at[cols, :]

    for k, j, kind in pieces:
        z = p.z_plus(j)
        cp.go(
            lambda: g_ref((g_up, g_down)[kind], kind, z, 1 - p.y, k),
            lambda: y_ref(kind, z, k),
            y_g.at[j, k, kind],
            p.at_y,
        )

    def gradient(k, j, kind):
        z = p.z_plus(j)
        landed(p, lambda: y_ref(kind, z, k), y_g.at[j, k, kind])
        add_into(y_ref(kind, z, k), g_ref((g_up, g_down)[kind], kind, z, p.y, k), dr if kind == 0 else fch, 64)
        if j == 0:
            cp.local(lambda: y_ref(kind, z, k), lambda: out_ref(kind, p.z, k))
        else:
            cp.go(
                lambda: y_ref(kind, z, k),
                lambda: out_ref(kind, p.z, k),
                z_g.at[j - 1, k, kind],
                lambda: p.at_z(z),
            )

    def core_stage(t, i):
        for j in range(X):
            x = p.x_plus(j + 1)
            landed(p, lambda: c_buf.at[i, t, x], c_s.at[i, t, j])
            add_into(c_buf.at[i, t, x], partial[i].at[rows_of(t, x, p.c), :], n, 16)
            if j < X - 1:
                cp.go(
                    lambda: c_buf.at[i, t, x],
                    lambda: x_buf.at[j, i, t],
                    x_s.at[j, i, t],
                    lambda: p.at_x(x),
                )

    def x_stage(t, i):
        for j in range(X - 1):
            landed(p, lambda: x_buf.at[j, i, t], x_s.at[j, i, t])
            add_into(c_buf.at[i, t, p.x], x_buf.at[j, i, t], n, 16)

    def chain(t, i, hop):
        if hop < t:
            here = p.z == hop
            if hop == 0:
                cp.go(
                    lambda: c_buf.at[i, t, p.x],
                    lambda: r_buf.at[i, t],
                    r_s.at[i, t],
                    lambda: p.at_z(p.z + 1),
                    here,
                )
            else:
                landed(p, lambda: r_buf.at[i, t], r_s.at[i, t], here)
                pl.when(here)(lambda: add_into(r_buf.at[i, t], c_buf.at[i, t, p.x], n, 16))
                cp.go(
                    lambda: r_buf.at[i, t],
                    lambda: r_buf.at[i, t],
                    r_s.at[i, t],
                    lambda: p.at_z(p.z + 1),
                    here,
                )
        low = Z - 1 - hop
        if low > t:
            here = p.z == low
            if hop == 0:
                cp.go(
                    lambda: c_buf.at[i, t, p.x],
                    lambda: l_buf.at[i, t],
                    l_s.at[i, t],
                    lambda: p.at_z(p.z - 1),
                    here,
                )
            else:
                landed(p, lambda: l_buf.at[i, t], l_s.at[i, t], here)
                pl.when(here)(lambda: add_into(l_buf.at[i, t], c_buf.at[i, t, p.x], n, 16))
                cp.go(
                    lambda: l_buf.at[i, t],
                    lambda: l_buf.at[i, t],
                    l_s.at[i, t],
                    lambda: p.at_z(p.z - 1),
                    here,
                )

    sums = [(t, i) for t in order for i in range(2)]
    pieces_left = list(pieces)

    def some_gradients(count):
        for _ in range(count):
            if pieces_left:
                gradient(*pieces_left.pop(0))

    for item in sums:
        core_stage(*item)
    lag = 2
    steps = len(sums) + lag * (Z - 2)
    per_step = 2
    for step in range(steps):
        some_gradients(per_step)
        if step < len(sums):
            x_stage(*sums[step])
        for hop in range(Z - 1):
            at = step - hop * lag
            if 0 <= at < len(sums):
                chain(*sums[at], hop)

    for i in range(2):
        for t in range(Z):
            here = p.z == t
            if t > 0:
                landed(p, lambda: r_buf.at[i, t], r_s.at[i, t], here)
            if t < Z - 1:
                landed(p, lambda: l_buf.at[i, t], l_s.at[i, t], here)

    def total(i, at):
        own = c_buf[i, p.z, p.x, at, :].astype(F32)
        right = r_buf[i, p.z, at, :].astype(F32)
        left = l_buf[i, p.z, at, :].astype(F32)
        right = right * (p.z > 0).astype(F32)
        left = left * (p.z < Z - 1).astype(F32)
        return own + right + left

    scale = 1.0 + levels[1:2, :]
    gate = levels[2:3, :]

    def last(b, _):
        at = pl.ds(pl.multiple_of(b * n_text, n_text), n_text)
        tokens = joined[at, :].astype(F32)
        back = d_out[at, :].astype(F32)
        centred = tokens - jnp.mean(tokens, axis=-1, keepdims=True)
        inv_std = lax.rsqrt(jnp.mean(centred * centred, axis=-1, keepdims=True) + EPS)
        normed = centred * inv_std
        fin[0, at, :] = (tokens + gate * total(0, at)).astype(BF16)
        d_normed = total(1, at) * scale
        d_full = back + inv_std * (
            d_normed
            - jnp.mean(d_normed, axis=-1, keepdims=True)
            - normed * jnp.mean(d_normed * normed, axis=-1, keepdims=True)
        )
        fin[1, at, :] = d_full.astype(BF16)

        @pl.when(b == 0)
        def _():
            null[0] = (d_full * drop[0:1, :]).astype(BF16)

        return 0

    lax.fori_loop(0, n // n_text, last, 0)

    def share(src, out, x_sem, c_sem):
        for j in range(1, X):
            cp.go(src, lambda: out(p.m), x_sem.at[j - 1], lambda j=j: p.at_x(p.x_plus(j)))
        cp.go(src, lambda: out(p.m), c_sem.at[0], p.at_c)
        cp.local(src, lambda: out(p.m))

    def relay(out, x_sem, c_sem):
        for j in range(1, X):
            quarter = lax.rem(p.x - j + X, X) * C + p.c
            landed(p, lambda: out(quarter), x_sem.at[j - 1])
            cp.go(lambda: out(quarter), lambda: out(quarter), c_sem.at[j], p.at_c)

    def settle(out, c_sem):
        for j in range(X):
            quarter = lax.rem(p.x - j + X, X) * C + 1 - p.c
            landed(p, lambda: out(quarter), c_sem.at[j])

    def fin_out(quarter):
        return fin_all.at[:, quarter]

    def null_out(quarter):
        return null_all.at[quarter]

    cp.go(lambda: null.at[0], lambda: null_y.at[...], n_y.at[0], p.at_y)
    share(lambda: fin.at[...], fin_out, f_x, f_c)
    some_gradients(2)
    landed(p, lambda: null_y.at[...], n_y.at[0])
    null[1] = (null[0].astype(F32) + null_y[...].astype(F32)).astype(BF16)
    for j in range(1, Z):
        cp.go(lambda: null.at[1], lambda: null_z.at[j - 1], n_z.at[j - 1], lambda: p.at_z(p.z_plus(j)))
    some_gradients(len(pieces))
    for j in range(1, Z):
        landed(p, lambda: null_z.at[j - 1], n_z.at[j - 1])
    whole_null = null[1].astype(F32)
    for j in range(1, Z):
        whole_null = whole_null + null_z[j - 1].astype(F32)
    null[2] = whole_null.astype(BF16)
    share(lambda: null.at[2], null_out, n_x, n_c)
    relay(fin_out, f_x, f_c)
    relay(null_out, n_x, n_c)
    settle(fin_out, f_c)
    settle(null_out, n_c)
    for k, j, kind in pieces:
        if j > 0:
            z = lax.rem(p.z - j + Z, Z)
            landed(p, lambda: out_ref(kind, z, k), z_g.at[j - 1, k, kind])
    cp.finish()


def shards(
    dp,
    mp,
    image_tokens,
    text_tokens,
    null_prompt,
    drop_flags,
    time_index,
    modulation,
    w_up,
    w_down,
    d_output,
):
    Z, X = dp // Y, mp // C
    d_rows, ff_m = w_up.shape
    fz = ff_m // Z
    nch = fz // 256
    width = d_rows * dp
    all_text = text_tokens.shape[1]
    n_text = all_text // mp
    n_image = image_tokens.shape[1] // mp
    n = n_text + n_image
    m = lax.axis_index("mp")

    def share(text_part, image_part):
        t = lax.dynamic_slice_in_dim(text_part, m * n_text, n_text, 0)
        i = lax.dynamic_slice_in_dim(image_part, m * n_image, n_image, 0)
        return jnp.concatenate([t, i], axis=0)

    dropped = drop_flags[0] == 1
    joined = share(jnp.where(dropped, null_prompt, text_tokens[0]), image_tokens[0])
    d_out = share(d_output[0, :all_text], d_output[0, all_text:])
    level = lax.dynamic_index_in_dim(modulation, time_index[0], 0, keepdims=False)
    joined32 = joined.astype(F32)
    shift, scale, gate = level[0][None], level[1][None], level[2][None]
    centred = joined32 - jnp.mean(joined32, axis=-1, keepdims=True)
    inv_std = lax.rsqrt(jnp.mean(centred * centred, axis=-1, keepdims=True) + EPS)
    mod_in = (centred * inv_std * (1.0 + scale) + shift).astype(BF16)
    d_branch = (d_out.astype(F32) * gate).astype(BF16)
    own = jnp.stack([mod_in, d_branch])

    anywhere = pl.BlockSpec(memory_space=pl.ANY)
    vmem = pl.BlockSpec(memory_space=pltpu.VMEM)
    dma = pltpu.SemaphoreType.DMA
    slots = 1 + 2 * (Z - 1)
    sends = (
        slots * X
        + 2 * (Z - 1)
        + 4 * nch * Z
        + 2 * nch
        + 1
        + slots * X
    )
    tok, up, down = pl.pallas_call(
        functools.partial(arrive, dp, mp, nch),
        out_shape=(
            jax.ShapeDtypeStruct((2, Z, mp, n, width), BF16),
            jax.ShapeDtypeStruct((width, fz), BF16),
            jax.ShapeDtypeStruct((fz, width), BF16),
        ),
        in_specs=[anywhere] * 3,
        out_specs=(anywhere,) * 3,
        scratch_shapes=[
            dma((sends,)),
            dma((2, Z - 1)),
            dma((max(X - 1, 1), slots)),
            dma((X, slots)),
            dma((Z - 1, nch, 2)),
            dma((Z, nch, 2)),
        ],
        compiler_params=pltpu.CompilerParams(collective_id=0, has_side_effects=True),
    )(own, w_up, w_down)

    rows = Z * mp * n
    tokens = tok[0].reshape(rows, width)
    d_tok = tok[1].reshape(rows, width)
    pre = dot(tokens, up, ((1,), (0,)))
    hid, back = jax.vjp(gelu_tanh, pre)
    d_hid = dot(d_tok, down, ((1,), (1,)))
    hid = hid.astype(BF16)
    d_pre = back(d_hid)[0].astype(BF16)
    branch = dot(hid, down, ((1,), (0,))).astype(BF16)
    d_mod = dot(d_pre, up, ((1,), (1,))).astype(BF16)
    g_up = dot(tokens, d_pre, ((0,), (0,))).astype(BF16)
    g_down = dot(hid, d_tok, ((0,), (0,))).astype(BF16)

    drop = jnp.where(dropped, jnp.ones((8, width), F32), jnp.zeros((8, width), F32))
    sends = (
        2 * Z * X
        + 4 * nch * Z
        + 2 * Z * (X - 1)
        + 4 * Z * (Z - 1)
        + 1
        + (Z - 1)
        + 2 * (X + 1)
        + 2 * (X - 1)
    )
    fin_all, null_all, up_out, down_out = pl.pallas_call(
        functools.partial(depart, dp, mp, nch, n_text),
        out_shape=(
            jax.ShapeDtypeStruct((2, mp, n, width), BF16),
            jax.ShapeDtypeStruct((mp, n_text, width), BF16),
            jax.ShapeDtypeStruct((d_rows, ff_m), BF16),
            jax.ShapeDtypeStruct((ff_m, d_rows), BF16),
        ),
        in_specs=[vmem] * 8,
        out_specs=(anywhere,) * 4,
        scratch_shapes=[
            pltpu.VMEM((Z * d_rows, fz), BF16),
            pltpu.VMEM((fz, Z * d_rows), BF16),
            pltpu.VMEM((2, Z, X, n, width), BF16),
            pltpu.VMEM((X - 1, 2, Z, n, width), BF16),
            pltpu.VMEM((2, Z, n, width), BF16),
            pltpu.VMEM((2, Z, n, width), BF16),
            pltpu.VMEM((2, n, width), BF16),
            pltpu.VMEM((3, n_text, width), BF16),
            pltpu.VMEM((n_text, width), BF16),
            pltpu.VMEM((Z - 1, n_text, width), BF16),
            dma((sends,)),
            dma((Z, nch, 2)),
            dma((Z - 1, nch, 2)),
            dma((2, Z, X)),
            dma((X - 1, 2, Z)),
            dma((2, Z)),
            dma((2, Z)),
            dma((X - 1,)),
            dma((X,)),
            dma((1,)),
            dma((Z - 1,)),
            dma((X - 1,)),
            dma((X,)),
        ],
        compiler_params=pltpu.CompilerParams(
            collective_id=1, has_side_effects=True, vmem_limit_bytes=62 * 1024 * 1024
        ),
    )(g_up, g_down, branch, d_mod, joined, d_out, level, drop)

    def whole(every):
        text = every[:, :n_text].reshape(-1, width)
        image = every[:, n_text:].reshape(-1, width)
        return jnp.concatenate([text, image], axis=0)[None]

    return (
        whole(fin_all[0]),
        whole(fin_all[1]),
        up_out.astype(F32),
        down_out.astype(F32),
        null_all.reshape(-1, width).astype(F32),
    )


def fits(dp, mp, image_tokens, text_tokens, w_up):
    d_rows, ff_m = w_up.shape
    return (
        dp % Y == 0
        and dp // Y > 1
        and mp % C == 0
        and mp // C > 1
        and d_rows % 128 == 0
        and ff_m % (dp // Y * 256) == 0
        and text_tokens.shape[1] % (mp * 16) == 0
        and image_tokens.shape[1] % text_tokens.shape[1] == 0
    )


def program(dp, mp, image_tokens, text_tokens, null_prompt, drop_flags, time_index, modulation, w_up, w_down, d_output):
    path = shards if fits(dp, mp, image_tokens, text_tokens, w_up) else generic
    return path(
        dp, mp, image_tokens, text_tokens, null_prompt, drop_flags, time_index, modulation, w_up, w_down, d_output
    )


def solution(mesh):
    placed = (
        P("dp", None, None),
        P("dp", None, None),
        P(),
        P("dp"),
        P("dp"),
        P(),
        P("dp", "mp"),
        P("mp", "dp"),
        P("dp", None, None),
    )
    return jax.shard_map(
        functools.partial(program, mesh.shape["dp"], mesh.shape["mp"]),
        mesh=mesh,
        in_specs=placed,
        out_specs=(P("dp", None, None), P("dp", None, None), P("dp", "mp"), P("mp", "dp"), P()),
        check_vma=False,
    )
```

```python
import functools

import jax
import jax.numpy as jnp
from jax import lax
from jax.experimental import pallas as pl
from jax.experimental.pallas import tpu as pltpu
from jax.sharding import PartitionSpec as P

EPS = 1e-06
BF16 = jnp.bfloat16
F32 = jnp.float32
MESH = pl.DeviceIdType.MESH
Y = 2
C = 2


def gelu_tanh(values):
    return jax.nn.gelu(values, approximate=True)


def dot(left, right, dims):
    return lax.dot_general(left, right, (dims, ((), ())), preferred_element_type=F32)


def swap(values, axis, size, bit):
    return lax.ppermute(values, axis, [(i, i ^ bit) for i in range(size)])


def generic(
    dp,
    mp,
    image_tokens,
    text_tokens,
    null_prompt,
    drop_flags,
    time_index,
    modulation,
    w_up,
    w_down,
    d_output,
):
    lines = [list(range(parity, dp, 2)) for parity in range(2)]
    per_line = dp // 2
    bits = []
    bit = 1
    while bit < mp:
        bits.append(bit)
        bit *= 2

    d_rows, ff_m = w_up.shape
    f = ff_m // dp
    width = d_rows * dp

    up_own = lax.all_to_all(
        w_up.reshape(d_rows, dp, f).transpose(1, 0, 2), "dp", 0, 0, tiled=True
    ).reshape(width, f)
    down_own = (
        lax.all_to_all(w_down.reshape(dp, f, d_rows), "dp", 0, 0, tiled=True)
        .transpose(1, 0, 2)
        .reshape(f, width)
    )
    up_other = swap(up_own, "dp", dp, 1)
    down_other = swap(down_own, "dp", dp, 1)

    m = lax.axis_index("mp")
    n_text = text_tokens.shape[1] // mp
    n_image = image_tokens.shape[1] // mp
    all_text = text_tokens.shape[1]

    def share(text_part, image_part):
        t = lax.dynamic_slice_in_dim(text_part, m * n_text, n_text, 0)
        i = lax.dynamic_slice_in_dim(image_part, m * n_image, n_image, 0)
        return jnp.concatenate([t, i], axis=0)

    dropped = drop_flags[0] == 1
    joined32 = share(
        jnp.where(dropped, null_prompt, text_tokens[0]), image_tokens[0]
    ).astype(F32)
    d_out32 = share(d_output[0, :all_text], d_output[0, all_text:]).astype(F32)
    level = lax.dynamic_index_in_dim(modulation, time_index[0], 0, keepdims=False)
    shift, scale, gate = level[0][None], level[1][None], level[2][None]
    centred = joined32 - jnp.mean(joined32, axis=-1, keepdims=True)
    inv_std = lax.rsqrt(jnp.mean(centred * centred, axis=-1, keepdims=True) + EPS)
    normed = centred * inv_std
    mod_in = (normed * (1.0 + scale) + shift).astype(BF16)
    d_branch = (d_out32 * gate).astype(BF16)

    def gather(rows):
        rows = lax.all_gather(rows, "dp", axis=0, tiled=True, axis_index_groups=lines)
        for b in reversed(bits):
            rows = jnp.concatenate([rows, swap(rows, "mp", mp, b)], axis=0)
        return rows

    def scatter(own, other, block_own, block_other, contract):
        def product(rows):
            return dot(own[rows], block_own, contract) + dot(other[rows], block_other, contract)

        half = own.shape[0] // 2
        sent = swap(product(slice(half, None)).astype(BF16), "mp", mp, bits[0])
        total = product(slice(0, half)) + sent.astype(F32)
        for b in bits[1:]:
            half = total.shape[0] // 2
            total = total[:half] + swap(total[half:].astype(BF16), "mp", mp, b).astype(F32)
        parts = lax.all_to_all(
            total.astype(BF16).reshape(per_line, -1, width),
            "dp",
            0,
            0,
            tiled=True,
            axis_index_groups=lines,
        )
        return jnp.sum(parts.astype(F32), axis=0)

    tokens = gather(mod_in)
    d_tok = gather(d_branch)

    def half_block(up, down):
        pre = dot(tokens, up, ((1,), (0,)))
        hid, back = jax.vjp(gelu_tanh, pre)
        d_hid = dot(d_tok, down, ((1,), (1,)))
        return hid.astype(BF16), back(d_hid)[0].astype(BF16)

    hid_own, dpre_own = half_block(up_own, down_own)
    hid_other, dpre_other = half_block(up_other, down_other)
    branch = scatter(hid_own, hid_other, down_own, down_other, ((1,), (0,)))
    d_mod = scatter(dpre_own, dpre_other, up_own, up_other, ((1,), (1,)))

    up_sent = dot(tokens, dpre_other, ((0,), (0,))).astype(BF16)
    down_sent = dot(hid_other, d_tok, ((0,), (0,))).astype(BF16)
    up_back = swap(up_sent, "dp", dp, 1)
    down_back = swap(down_sent, "dp", dp, 1)
    g_up = dot(tokens, dpre_own, ((0,), (0,))) + up_back.astype(F32)
    g_down = dot(hid_own, d_tok, ((0,), (0,))) + down_back.astype(F32)
    grad_up = (
        lax.all_to_all(g_up.astype(BF16).reshape(dp, d_rows, f), "dp", 0, 0, tiled=True)
        .transpose(1, 0, 2)
        .reshape(d_rows, ff_m)
        .astype(F32)
    )
    grad_down = (
        lax.all_to_all(
            g_down.astype(BF16).reshape(f, dp, d_rows).transpose(1, 0, 2),
            "dp",
            0,
            0,
            tiled=True,
        )
        .reshape(ff_m, d_rows)
        .astype(F32)
    )

    block_out = (joined32 + gate * branch).astype(BF16)
    d_normed = d_mod * (1.0 + scale)
    d_full = d_out32 + inv_std * (
        d_normed
        - jnp.mean(d_normed, axis=-1, keepdims=True)
        - normed * jnp.mean(d_normed * normed, axis=-1, keepdims=True)
    )
    null_part = jnp.where(dropped, d_full[:n_text], F32(0.0)).astype(BF16)
    null_sum = lax.psum(null_part, "dp")

    def whole(rows):
        every = lax.all_gather(rows, "mp", axis=0)
        return jnp.concatenate(
            [
                every[:, :n_text].reshape(-1, width),
                every[:, n_text:].reshape(-1, width),
            ],
            axis=0,
        )[None]

    grad_null = lax.all_gather(null_sum, "mp", axis=0, tiled=True).astype(F32)
    return (whole(block_out), whole(d_full.astype(BF16)), grad_up, grad_down, grad_null)


class Place:
    def __init__(self, dp, mp):
        self.Z, self.X = dp // Y, mp // C
        d, m = lax.axis_index("dp"), lax.axis_index("mp")
        self.z, self.y = d // Y, d % Y
        self.x, self.c = m // C, m % C
        self.d, self.m = d, m

    def at_z(self, z):
        return (z * Y + self.y, self.m)

    def at_y(self):
        return (self.z * Y + 1 - self.y, self.m)

    def at_x(self, x):
        return (self.d, x * C + self.c)

    def at_c(self):
        return (self.d, self.x * C + 1 - self.c)

    def z_plus(self, j):
        return lax.rem(self.z + j, self.Z)

    def x_plus(self, j):
        return lax.rem(self.x + j, self.X)

    def meet(self):
        barrier = pltpu.get_barrier_semaphore()
        peers = [self.at_z(self.z_plus(j)) for j in range(1, self.Z)]
        peers += [self.at_x(self.x_plus(j)) for j in range(1, self.X)]
        peers += [self.at_y(), self.at_c()]
        for peer in peers:
            pl.semaphore_signal(barrier, inc=1, device_id=peer, device_id_type=MESH)
        pl.semaphore_wait(barrier, len(peers))


class Copies:
    def __init__(self, sems):
        self.sems, self.used, self.open = sems, 0, []

    def go(self, src, dst, recv, device, when=None):
        sem = self.sems.at[self.used]
        self.used += 1

        source, target, peer = src(), dst(), device()

        def make():
            return pltpu.make_async_remote_copy(
                src_ref=source,
                dst_ref=target,
                send_sem=sem,
                recv_sem=recv,
                device_id=peer,
                device_id_type=MESH,
            )

        def start():
            make().start()

        def finish():
            make().wait_send()

        guard(when, start)
        self.open.append((when, finish))

    def local(self, src, dst, when=None):
        sem = self.sems.at[self.used]
        self.used += 1

        source, target = src(), dst()

        def make():
            return pltpu.make_async_copy(source, target, sem)

        def start():
            make().start()

        def finish():
            make().wait()

        guard(when, start)
        self.open.append((when, finish))

    def finish(self):
        for when, wait in self.open:
            guard(when, wait)
        self.open = []


def guard(when, act):
    if when is None:
        act()
    else:
        pl.when(when)(act)


def landed(place, ref, recv, when=None):
    def act():
        pltpu.make_async_remote_copy(
            src_ref=ref(),
            dst_ref=ref(),
            send_sem=recv,
            recv_sem=recv,
            device_id=place.at_y(),
            device_id_type=MESH,
        ).wait_recv()

    guard(when, act)


def tile(index, size):
    return pl.ds(pl.multiple_of(index * size, size), size)


def add_into(target, other, rows, step):
    def body(i, _):
        at = pl.ds(pl.multiple_of(i * step, step), step)
        target[at, :] = (target[at, :].astype(F32) + other[at, :].astype(F32)).astype(BF16)
        return 0

    lax.fori_loop(0, rows // step, body, 0)


def each(first, last, act):
    def body(i, _):
        act(i)
        return 0

    lax.fori_loop(first, last, body, 0)


def block_kernel(
    dp,
    mp,
    nch,
    drop,
    level,
    image,
    text,
    null_prompt,
    d_output,
    w_up,
    w_down,
    out_all,
    d_tok_all,
    null_all,
    up_out,
    down_out,
    joined,
    text_v,
    null_v,
    d_out,
    tok,
    up,
    down,
    hid,
    d_pre,
    g_up,
    g_down,
    y_up,
    y_down,
    s_buf,
    c_buf,
    x_buf,
    l_buf,
    fin,
    null,
    null_y,
    null_z,
    send,
    z_tok,
    x_tok,
    c_tok,
    z_w,
    y_w,
    y_out,
    y_g,
    z_out,
    z_g,
    c_s,
    x_s,
    r_s,
    l_s,
    f_x,
    f_c,
    n_y,
    n_z,
    n_x,
    n_c,
    loads,
):
    p = Place(dp, mp)
    Z, X = p.Z, p.X
    dr = w_up.shape[0]
    fz = w_up.shape[1] // Z
    fch = fz // nch
    width = dr * dp
    n_text, n_image = text.shape[1] // mp, image.shape[1] // mp
    n = n_text + n_image
    half = Z * X * n
    rows = C * half
    cp = Copies(send)
    far = [2, 1, 3] if Z == 4 else list(range(1, Z))

    def at_rows(c, z, x):
        return pl.ds(pl.multiple_of(((c * Z + z) * X + x) * n, n), n)

    every_text = text.shape[1]
    text_at = pl.ds(pl.multiple_of(p.m * n_text, n_text), n_text)
    image_at = pl.ds(pl.multiple_of(p.m * n_image, n_text), n_image)
    later = pl.ds(pl.multiple_of(every_text + p.m * n_image, n_text), n_image)
    first = [
        pltpu.make_async_copy(text.at[0, text_at], text_v, loads.at[0]),
        pltpu.make_async_copy(null_prompt.at[text_at], null_v, loads.at[1]),
        pltpu.make_async_copy(image.at[0, image_at], joined.at[pl.ds(n_text, n_image)], loads.at[2]),
        pltpu.make_async_copy(d_output.at[0, text_at], d_out.at[pl.ds(0, n_text)], loads.at[3]),
        pltpu.make_async_copy(d_output.at[0, later], d_out.at[pl.ds(n_text, n_image)], loads.at[4]),
    ]
    for copy in first:
        copy.start()
    p.meet()

    def up_src(z, k):
        return w_up.at[:, pl.ds(pl.multiple_of(z * fz + k * fch, fch), fch)]

    def down_src(z, k):
        return w_down.at[pl.ds(pl.multiple_of(z * fz + k * fch, fch), fch), :]

    def up_dst(d, k):
        return up.at[tile(d, dr), pl.ds(k * fch, fch)]

    def down_dst(d, k):
        return down.at[pl.ds(k * fch, fch), tile(d, dr)]

    kinds = ((up_src, up_dst), (down_src, down_dst))

    def z_weights(k, which):
        for j in which:
            for kind, (src, dst) in enumerate(kinds):
                cp.go(
                    lambda: src(p.z_plus(j), k),
                    lambda: dst(p.d, k),
                    z_w.at[j - 1, k, kind],
                    lambda: p.at_z(p.z_plus(j)),
                )

    def forward(k, j):
        d_src = lax.rem(p.z - j + Z, Z) * Y + p.y
        for kind, (_, dst) in enumerate(kinds):
            landed(p, lambda: dst(d_src, k), z_w.at[j - 1, k, kind])
            cp.go(lambda: dst(d_src, k), lambda: dst(d_src, k), y_w.at[j, k, kind], p.at_y)

    def weights_here(k):
        for j in range(Z):
            d_src = lax.rem(p.z - j + Z, Z) * Y + 1 - p.y
            for kind, (_, dst) in enumerate(kinds):
                landed(p, lambda: dst(d_src, k), y_w.at[j, k, kind])

    own_weights = []
    for k in range(nch):
        for kind, (src, dst) in enumerate(kinds):
            cp.go(lambda: src(p.z, k), lambda: dst(p.d, k), y_w.at[0, k, kind], p.at_y)
            copy = pltpu.make_async_copy(src(p.z, k), dst(p.d, k), loads.at[5 + 2 * k + kind])
            copy.start()
            own_weights.append(copy)

    for copy in first:
        copy.wait()
    joined[pl.ds(0, n_text)] = jnp.where(drop[0] == 1, null_v[...], text_v[...])
    shift, scale, gate = level[0:1, :], 1.0 + level[1:2, :], level[2:3, :]

    def stats(at):
        values = joined[at, :].astype(F32)
        centred = values - jnp.mean(values, axis=-1, keepdims=True)
        inv_std = lax.rsqrt(jnp.mean(centred * centred, axis=-1, keepdims=True) + EPS)
        return values, centred * inv_std, inv_std

    mine = pl.multiple_of(((p.c * Z + p.z) * X + p.x) * n, n)

    def prepare(b):
        at = pl.ds(pl.multiple_of(b * n_text, n_text), n_text)
        to = pl.ds(pl.multiple_of(mine + b * n_text, n_text), n_text)
        _, normed, _ = stats(at)
        tok[0, to, :] = (normed * scale + shift).astype(BF16)
        tok[1, to, :] = (d_out[at, :].astype(F32) * gate).astype(BF16)

    each(0, n // n_text, prepare)

    slots = [(0, p.z, None)]
    for s in range(Z - 1):
        slots.append((1 + 2 * s, p.z - 1 - s, p.z - 1 - s >= 0))
        slots.append((2 + 2 * s, p.z + 1 + s, p.z + 1 + s < Z))

    def block(sample, x, c):
        return tok.at[:, at_rows(c, sample, x), :]

    def spread(slot, sample, when):
        def ref():
            return block(sample, p.x, p.c)

        for j in range(1, X):
            cp.go(ref, ref, x_tok.at[j - 1, slot], lambda: p.at_x(p.x_plus(j)), when)
        cp.go(ref, ref, c_tok.at[0, slot], p.at_c, when)

    def pass_on(s, i):
        for way in (1, -1):
            sample = p.z - s * way
            inside = (sample >= 0) & (p.z + 1 < Z) if way == 1 else (sample < Z) & (p.z >= 1)

            def ref():
                return tok.at[i, at_rows(p.c, sample, p.x), :]

            cp.go(ref, ref, z_tok.at[(0 if way == 1 else 1), s, i], lambda: p.at_z(p.z + way), inside)

    for i in range(2):
        pass_on(0, i)
    spread(*slots[0])
    for s in range(Z - 1):
        for i in range(2):
            for side in (0, 1):
                slot, sample, valid = slots[1 + 2 * s + side]
                landed(p, lambda: tok.at[i, at_rows(p.c, sample, p.x), :], z_tok.at[side, s, i], valid)
            if s < Z - 2:
                pass_on(s + 1, i)
        if s == min(1, Z - 2):
            z_weights(0, far)
        for side in (0, 1):
            spread(*slots[1 + 2 * s + side])
    z_weights(1, far)
    for j in far:
        forward(0, j)
    for slot, sample, valid in slots:
        for j in range(1, X):
            x = lax.rem(p.x - j + X, X)

            def ref():
                return block(sample, x, p.c)

            landed(p, ref, x_tok.at[j - 1, slot], valid)
            cp.go(ref, ref, c_tok.at[j, slot], p.at_c, valid)
    for k in range(2, nch):
        z_weights(k, far)
    for slot, sample, valid in slots:
        for j in range(X):
            x = lax.rem(p.x - j + X, X)
            landed(p, lambda: block(sample, x, 1 - p.c), c_tok.at[j, slot], valid)

    tall = 256

    def hidden(k):
        units = pl.ds(k * fch, fch)

        def act(r):
            at = pl.ds(pl.multiple_of(r * tall, tall), tall)
            pre = dot(tok[0, at, :], up[:, units], ((1,), (0,)))
            d_hid = dot(tok[1, at, :], down[units, :], ((1,), (1,)))
            values, back = jax.vjp(gelu_tanh, pre)
            hid[at, units] = values.astype(BF16)
            d_pre[at, units] = back(d_hid)[0].astype(BF16)

        each(0, rows // tall, act)

    def y_copy(i, kind):
        k, j, z = place_of(i)
        ref = g_ref(kind, z, k)
        return pltpu.make_async_remote_copy(
            src_ref=ref((g_up, g_down)[kind]),
            dst_ref=ref((y_up, y_down)[kind]),
            send_sem=y_out.at[j, k, kind],
            recv_sem=y_g.at[j, k, kind],
            device_id=p.at_y(),
            device_id_type=MESH,
        )

    def place_of(i):
        k = i // Z
        j = lax.rem(i - k * Z + Z // 2, Z)
        return k, j, p.z_plus(j)

    def units_of(k):
        return pl.ds(pl.multiple_of(k * fch, fch), fch)

    def g_ref(kind, z, k):
        def ref(buffer):
            return buffer.at[tile(z, dr), units_of(k)] if kind == 0 else buffer.at[units_of(k), tile(z, dr)]

        return ref

    def product(kind, z, y, k):
        features = tile(z * Y + y, dr)
        if kind == 0:
            return dot(tok[0, :, features], d_pre[:, units_of(k)], ((0,), (0,)))
        return dot(hid[:, units_of(k)], tok[1, :, features], ((0,), (0,)))

    def peer_gradient(i):
        k, j, z = place_of(i)
        for kind in range(2):
            g_ref(kind, z, k)((g_up, g_down)[kind])[...] = product(kind, z, 1 - p.y, k).astype(BF16)
            y_copy(i, kind).start()

    def out_ref(kind, z, k):
        cols = pl.ds(pl.multiple_of(z * fz + k * fch, fch), fch)
        return up_out.at[:, cols] if kind == 0 else down_out.at[cols, :]

    def z_copy(i, kind):
        k, j, z = place_of(i)
        return pltpu.make_async_remote_copy(
            src_ref=g_ref(kind, z, k)((y_up, y_down)[kind]),
            dst_ref=out_ref(kind, p.z, k),
            send_sem=z_out.at[j, k, kind],
            recv_sem=z_g.at[j, k, kind],
            device_id=p.at_z(z),
            device_id_type=MESH,
        )

    def kept(i, kind):
        k, j, z = place_of(i)
        return pltpu.make_async_copy(
            g_ref(kind, z, k)((y_up, y_down)[kind]), out_ref(kind, p.z, k), z_out.at[j, k, kind]
        )

    def own_gradient(i):
        k, j, z = place_of(i)
        for kind in range(2):
            y_copy(i, kind).wait_recv()
            ref = g_ref(kind, z, k)((y_up, y_down)[kind])
            ref[...] = (product(kind, z, p.y, k) + ref[...].astype(F32)).astype(BF16)
            pl.when(j > 0)(lambda: z_copy(i, kind).start())
            pl.when(j == 0)(lambda: kept(i, kind).start())

    count = nch * Z
    started, ended = [0], [0]

    def some_peer(number):
        last = min(count, started[0] + number)
        if last > started[0]:
            each(started[0], last, peer_gradient)
            started[0] = last

    def some_own(number):
        last = min(started[0], ended[0] + number)
        if last > ended[0]:
            each(ended[0], last, own_gradient)
            ended[0] = last

    for copy in own_weights:
        copy.wait()
    weights_here(0)
    hidden(0)
    for k in range(1, nch):
        for at, j in enumerate(far):
            forward(k, j)
            if at == (1 if k == 1 else 0):
                some_peer(1)
        if k == nch - 1:
            some_own(2)
            some_peer(k * Z - started[0])
        weights_here(k)
        if k == nch - 1:
            some_own(1)
        hidden(k)

    wide = 256

    def summand(i, c, b):
        at = pl.ds(pl.multiple_of(c * half, half), half)
        cols = pl.ds(pl.multiple_of(b * wide, wide), wide)
        if i == 0:
            return cols, dot(hid[at, :], down[:, cols], ((1,), (0,)))
        return cols, dot(d_pre[at, :], up[cols, :], ((1,), (1,)))

    order = []
    for i in range((Z + 1) // 2):
        order += [Z - 1 - i] + ([i] if i != Z - 1 - i else [])

    def sample_rows(t):
        return pl.ds(t * X * n, X * n)

    def c_copy(i, t):
        return pltpu.make_async_remote_copy(
            src_ref=s_buf.at[i, sample_rows(t), :],
            dst_ref=c_buf.at[i, sample_rows(t), :],
            send_sem=c_s.at[0, i, t],
            recv_sem=c_s.at[1, i, t],
            device_id=p.at_c(),
            device_id_type=MESH,
        )

    def x_rows(t, x):
        return pl.ds(pl.multiple_of((t * X + x) * n, n), n)

    def own_rows(t):
        return x_rows(t, p.x)

    for i in range(2):

        def other(b):
            cols, value = summand(i, 1 - p.c, b)
            s_buf[i, :, cols] = value.astype(BF16)

        each(0, width // wide, other)
        for t in order:
            c_copy(i, t).start()
        some_own(1)
        for t in order:
            c_copy(i, t).wait_recv()

        def mine_too(b):
            cols, value = summand(i, p.c, b)
            c_buf[i, :, cols] = (value + c_buf[i, :, cols].astype(F32)).astype(BF16)

        each(0, width // wide, mine_too)
        for t in order:
            for j in range(1, X):
                x = p.x_plus(j)
                cp.go(
                    lambda: c_buf.at[i, x_rows(t, x), :],
                    lambda: x_buf.at[j - 1, i, t],
                    x_s.at[j - 1, i, t],
                    lambda: p.at_x(x),
                )
        some_own(1)
        some_peer(2)
    some_peer(count)

    def x_stage(t, i):
        for j in range(X - 1):
            landed(p, lambda: x_buf.at[j, i, t], x_s.at[j, i, t])
            add_into(c_buf.at[i, own_rows(t), :], x_buf.at[j, i, t], n, 16)

    def chain(t, i, hop):
        for way, here_z, slot, sem in (
            (1, hop, t, r_s),
            (-1, Z - 1 - hop, t, l_s),
        ):
            if (t - here_z) * way <= 0:
                continue
            here = p.z == here_z
            target = Z if way == -1 and here_z - 1 == t else t
            if hop == 0:
                source = lambda: c_buf.at[i, own_rows(t), :]
            else:
                source = lambda: l_buf.at[i, t]
                landed(p, source, sem.at[i, t], here)
                pl.when(here)(lambda: add_into(l_buf.at[i, t], c_buf.at[i, own_rows(t), :], n, 16))
            cp.go(source, lambda: l_buf.at[i, target], sem.at[i, t], lambda: p.at_z(here_z + way), here)

    is_dropped = (drop[0] == 1).astype(F32)

    def arrived(i):
        for t in range(Z):
            here = p.z == t
            if t > 0:
                landed(p, lambda: l_buf.at[i, t], r_s.at[i, t], here)
            if t < Z - 1:
                landed(p, lambda: l_buf.at[i, Z], l_s.at[i, t], here)

    def total(i, b, at):
        mine_at = pl.ds(pl.multiple_of((p.z * X + p.x) * n + b * n_text, n_text), n_text)
        own = c_buf[i, mine_at, :].astype(F32)
        low = l_buf[i, p.z, at, :].astype(F32)
        high = l_buf[i, Z, at, :].astype(F32)
        return own + jnp.where(p.z > 0, low, 0.0) + jnp.where(p.z < Z - 1, high, 0.0)

    def output(b):
        at = pl.ds(pl.multiple_of(b * n_text, n_text), n_text)
        fin[0, at, :] = (joined[at, :].astype(F32) + gate * total(0, b, at)).astype(BF16)

    def input_gradient(b):
        at = pl.ds(pl.multiple_of(b * n_text, n_text), n_text)
        _, normed, inv_std = stats(at)
        d_normed = total(1, b, at) * scale
        d_full = d_out[at, :].astype(F32) + inv_std * (
            d_normed
            - jnp.mean(d_normed, axis=-1, keepdims=True)
            - normed * jnp.mean(d_normed * normed, axis=-1, keepdims=True)
        )
        fin[1, at, :] = d_full.astype(BF16)

        @pl.when(b == 0)
        def _():
            null[0] = (d_full * is_dropped).astype(BF16)

    def share(src, out, x_sem, c_sem):
        for j in range(1, X):
            cp.go(src, lambda: out(p.m), x_sem.at[j - 1], lambda: p.at_x(p.x_plus(j)))
        cp.go(src, lambda: out(p.m), c_sem.at[0], p.at_c)
        cp.local(src, lambda: out(p.m))

    def relay(out, x_sem, c_sem):
        for j in range(1, X):
            quarter = lax.rem(p.x - j + X, X) * C + p.c
            landed(p, lambda: out(quarter), x_sem.at[j - 1])
            cp.go(lambda: out(quarter), lambda: out(quarter), c_sem.at[j], p.at_c)

    def settle(out, c_sem):
        for j in range(X):
            quarter = lax.rem(p.x - j + X, X) * C + 1 - p.c
            landed(p, lambda: out(quarter), c_sem.at[j])

    outs = [lambda quarter: out_all.at[quarter], lambda quarter: d_tok_all.at[quarter]]

    def null_out(quarter):
        return null_all.at[quarter]

    sums = [(t, i) for i in range(2) for t in order]
    lag = 2
    steps = len(sums) + lag * (Z - 2)
    for step in range(steps):
        if step % 2 == 0:
            some_own(1)
        if step < len(sums):
            x_stage(*sums[step])
        for hop in range(Z - 1):
            at = step - hop * lag
            if 0 <= at < len(sums):
                chain(*sums[at], hop)
        if step == Z + lag * (Z - 2) + 1:
            arrived(0)
            each(0, n // n_text, output)
            share(lambda: fin.at[0], outs[0], f_x.at[0], f_c.at[0])
    arrived(1)
    each(0, n // n_text, input_gradient)

    cp.go(lambda: null.at[0], lambda: null_y.at[...], n_y.at[0], p.at_y)
    share(lambda: fin.at[1], outs[1], f_x.at[1], f_c.at[1])
    relay(outs[0], f_x.at[0], f_c.at[0])
    landed(p, lambda: null_y.at[...], n_y.at[0])
    null[1] = (null[0].astype(F32) + null_y[...].astype(F32)).astype(BF16)
    for j in range(1, Z):
        cp.go(lambda: null.at[1], lambda: null_z.at[j - 1], n_z.at[j - 1], lambda: p.at_z(p.z_plus(j)))
    some_peer(count)
    some_own(count)
    relay(outs[1], f_x.at[1], f_c.at[1])
    for j in range(1, Z):
        landed(p, lambda: null_z.at[j - 1], n_z.at[j - 1])
    whole_null = null[1].astype(F32)
    for j in range(1, Z):
        whole_null = whole_null + null_z[j - 1].astype(F32)
    null[2] = whole_null.astype(BF16)
    share(lambda: null.at[2], null_out, n_x, n_c)
    relay(null_out, n_x, n_c)
    for i in range(2):
        settle(outs[i], f_c.at[i])
    settle(null_out, n_c)

    def settled(i):
        k, j, z = place_of(i)
        for kind in range(2):
            y_copy(i, kind).wait_send()

            @pl.when(j > 0)
            def _():
                source = lax.rem(p.z - j + Z, Z)
                landed(p, lambda: out_ref(kind, source, k), z_g.at[j, k, kind])
                z_copy(i, kind).wait_send()

            pl.when(j == 0)(lambda: kept(i, kind).wait())

    each(0, count, settled)
    for i in range(2):
        for t in range(Z):
            c_copy(i, t).wait_send()
    cp.finish()


def shards(
    dp,
    mp,
    image_tokens,
    text_tokens,
    null_prompt,
    drop_flags,
    time_index,
    modulation,
    w_up,
    w_down,
    d_output,
):
    Z, X = dp // Y, mp // C
    d_rows, ff_m = w_up.shape
    fz = ff_m // Z
    nch = fz // 256
    width = d_rows * dp
    n_text = text_tokens.shape[1] // mp
    n = n_text + image_tokens.shape[1] // mp
    rows = Z * mp * n
    level = lax.dynamic_index_in_dim(modulation, time_index[0], 0, keepdims=False)

    anywhere = pl.BlockSpec(memory_space=pl.ANY)
    dma = pltpu.SemaphoreType.DMA
    slots = 1 + 2 * (Z - 1)
    sends = (
        2 * nch * Z
        + slots * (2 * X - 1)
        + 4 * (Z - 1)
        + 2 * nch * Z
        + 2 * Z * (X - 1)
        + 2 * 2 * Z * (Z - 1)
        + 1
        + (Z - 1)
        + 3 * (X + 1)
        + 3 * (X - 1)
    )
    every_out, every_d_tok, every_null, up_out, down_out = pl.pallas_call(
        functools.partial(block_kernel, dp, mp, nch),
        out_shape=(
            jax.ShapeDtypeStruct((mp, n, width), BF16),
            jax.ShapeDtypeStruct((mp, n, width), BF16),
            jax.ShapeDtypeStruct((mp, n_text, width), BF16),
            jax.ShapeDtypeStruct((d_rows, ff_m), BF16),
            jax.ShapeDtypeStruct((ff_m, d_rows), BF16),
        ),
        in_specs=[
            pl.BlockSpec(memory_space=pltpu.SMEM),
            pl.BlockSpec(memory_space=pltpu.VMEM),
        ]
        + [anywhere] * 6,
        out_specs=(anywhere,) * 5,
        scratch_shapes=[
            pltpu.VMEM((n, width), BF16),
            pltpu.VMEM((n_text, width), BF16),
            pltpu.VMEM((n_text, width), BF16),
            pltpu.VMEM((n, width), BF16),
            pltpu.VMEM((2, rows, width), BF16),
            pltpu.VMEM((width, fz), BF16),
            pltpu.VMEM((fz, width), BF16),
            pltpu.VMEM((rows, fz), BF16),
            pltpu.VMEM((rows, fz), BF16),
            pltpu.VMEM((Z * d_rows, fz), BF16),
            pltpu.VMEM((fz, Z * d_rows), BF16),
            pltpu.VMEM((Z * d_rows, fz), BF16),
            pltpu.VMEM((fz, Z * d_rows), BF16),
            pltpu.VMEM((2, rows // C, width), BF16),
            pltpu.VMEM((2, rows // C, width), BF16),
            pltpu.VMEM((X - 1, 2, Z, n, width), BF16),
            pltpu.VMEM((2, Z + 1, n, width), BF16),
            pltpu.VMEM((2, n, width), BF16),
            pltpu.VMEM((3, n_text, width), BF16),
            pltpu.VMEM((n_text, width), BF16),
            pltpu.VMEM((Z - 1, n_text, width), BF16),
            dma((sends,)),
            dma((2, Z - 1, 2)),
            dma((X - 1, slots)),
            dma((X, slots)),
            dma((Z - 1, nch, 2)),
            dma((Z, nch, 2)),
            dma((Z, nch, 2)),
            dma((Z, nch, 2)),
            dma((Z, nch, 2)),
            dma((Z, nch, 2)),
            dma((2, 2, Z)),
            dma((X - 1, 2, Z)),
            dma((2, Z)),
            dma((2, Z)),
            dma((2, X - 1)),
            dma((2, X)),
            dma((1,)),
            dma((Z - 1,)),
            dma((X - 1,)),
            dma((X,)),
            dma((5 + 2 * nch,)),
        ],
        compiler_params=pltpu.CompilerParams(
            collective_id=0, has_side_effects=True, vmem_limit_bytes=67043328
        ),
    )(drop_flags, level, image_tokens, text_tokens, null_prompt, d_output, w_up, w_down)

    def whole(every):
        text = every[:, :n_text].reshape(-1, width)
        image = every[:, n_text:].reshape(-1, width)
        return jnp.concatenate([text, image], axis=0)[None]

    return (
        whole(every_out),
        whole(every_d_tok),
        up_out.astype(F32),
        down_out.astype(F32),
        every_null.reshape(-1, width).astype(F32),
    )


def fits(dp, mp, image_tokens, text_tokens, w_up):
    d_rows, ff_m = w_up.shape
    return (
        dp % Y == 0
        and dp // Y > 1
        and mp % C == 0
        and mp // C > 1
        and d_rows % 128 == 0
        and ff_m % (dp // Y * 256) == 0
        and ff_m > dp // Y * 256
        and text_tokens.shape[1] % (mp * 16) == 0
        and image_tokens.shape[1] % text_tokens.shape[1] == 0
    )


def program(dp, mp, image_tokens, text_tokens, null_prompt, drop_flags, time_index, modulation, w_up, w_down, d_output):
    path = shards if fits(dp, mp, image_tokens, text_tokens, w_up) else generic
    return path(
        dp, mp, image_tokens, text_tokens, null_prompt, drop_flags, time_index, modulation, w_up, w_down, d_output
    )


def solution(mesh):
    placed = (
        P("dp", None, None),
        P("dp", None, None),
        P(),
        P("dp"),
        P("dp"),
        P(),
        P("dp", "mp"),
        P("mp", "dp"),
        P("dp", None, None),
    )
    return jax.shard_map(
        functools.partial(program, mesh.shape["dp"], mesh.shape["mp"]),
        mesh=mesh,
        in_specs=placed,
        out_specs=(P("dp", None, None), P("dp", None, None), P("dp", "mp"), P("mp", "dp"), P()),
        check_vma=False,
    )
```

```python
import functools

import jax
import jax.numpy as jnp
from jax import lax
from jax.experimental import pallas as pl
from jax.experimental.pallas import tpu as pltpu
from jax.sharding import PartitionSpec as P

EPS = 1e-06
BF16 = jnp.bfloat16
F32 = jnp.float32
MESH = pl.DeviceIdType.MESH
Y = 2
C = 2


def gelu_tanh(values):
    return jax.nn.gelu(values, approximate=True)


def dot(left, right, dims):
    return lax.dot_general(left, right, (dims, ((), ())), preferred_element_type=F32)


def swap(values, axis, size, bit):
    return lax.ppermute(values, axis, [(i, i ^ bit) for i in range(size)])


def generic(
    dp,
    mp,
    image_tokens,
    text_tokens,
    null_prompt,
    drop_flags,
    time_index,
    modulation,
    w_up,
    w_down,
    d_output,
):
    lines = [list(range(parity, dp, 2)) for parity in range(2)]
    per_line = dp // 2
    bits = []
    bit = 1
    while bit < mp:
        bits.append(bit)
        bit *= 2

    d_rows, ff_m = w_up.shape
    f = ff_m // dp
    width = d_rows * dp

    up_own = lax.all_to_all(
        w_up.reshape(d_rows, dp, f).transpose(1, 0, 2), "dp", 0, 0, tiled=True
    ).reshape(width, f)
    down_own = (
        lax.all_to_all(w_down.reshape(dp, f, d_rows), "dp", 0, 0, tiled=True)
        .transpose(1, 0, 2)
        .reshape(f, width)
    )
    up_other = swap(up_own, "dp", dp, 1)
    down_other = swap(down_own, "dp", dp, 1)

    m = lax.axis_index("mp")
    n_text = text_tokens.shape[1] // mp
    n_image = image_tokens.shape[1] // mp
    all_text = text_tokens.shape[1]

    def share(text_part, image_part):
        t = lax.dynamic_slice_in_dim(text_part, m * n_text, n_text, 0)
        i = lax.dynamic_slice_in_dim(image_part, m * n_image, n_image, 0)
        return jnp.concatenate([t, i], axis=0)

    dropped = drop_flags[0] == 1
    joined32 = share(
        jnp.where(dropped, null_prompt, text_tokens[0]), image_tokens[0]
    ).astype(F32)
    d_out32 = share(d_output[0, :all_text], d_output[0, all_text:]).astype(F32)
    level = lax.dynamic_index_in_dim(modulation, time_index[0], 0, keepdims=False)
    shift, scale, gate = level[0][None], level[1][None], level[2][None]
    centred = joined32 - jnp.mean(joined32, axis=-1, keepdims=True)
    inv_std = lax.rsqrt(jnp.mean(centred * centred, axis=-1, keepdims=True) + EPS)
    normed = centred * inv_std
    mod_in = (normed * (1.0 + scale) + shift).astype(BF16)
    d_branch = (d_out32 * gate).astype(BF16)

    def gather(rows):
        rows = lax.all_gather(rows, "dp", axis=0, tiled=True, axis_index_groups=lines)
        for b in reversed(bits):
            rows = jnp.concatenate([rows, swap(rows, "mp", mp, b)], axis=0)
        return rows

    def scatter(own, other, block_own, block_other, contract):
        def product(rows):
            return dot(own[rows], block_own, contract) + dot(other[rows], block_other, contract)

        half = own.shape[0] // 2
        sent = swap(product(slice(half, None)).astype(BF16), "mp", mp, bits[0])
        total = product(slice(0, half)) + sent.astype(F32)
        for b in bits[1:]:
            half = total.shape[0] // 2
            total = total[:half] + swap(total[half:].astype(BF16), "mp", mp, b).astype(F32)
        parts = lax.all_to_all(
            total.astype(BF16).reshape(per_line, -1, width),
            "dp",
            0,
            0,
            tiled=True,
            axis_index_groups=lines,
        )
        return jnp.sum(parts.astype(F32), axis=0)

    tokens = gather(mod_in)
    d_tok = gather(d_branch)

    def half_block(up, down):
        pre = dot(tokens, up, ((1,), (0,)))
        hid, back = jax.vjp(gelu_tanh, pre)
        d_hid = dot(d_tok, down, ((1,), (1,)))
        return hid.astype(BF16), back(d_hid)[0].astype(BF16)

    hid_own, dpre_own = half_block(up_own, down_own)
    hid_other, dpre_other = half_block(up_other, down_other)
    branch = scatter(hid_own, hid_other, down_own, down_other, ((1,), (0,)))
    d_mod = scatter(dpre_own, dpre_other, up_own, up_other, ((1,), (1,)))

    up_sent = dot(tokens, dpre_other, ((0,), (0,))).astype(BF16)
    down_sent = dot(hid_other, d_tok, ((0,), (0,))).astype(BF16)
    up_back = swap(up_sent, "dp", dp, 1)
    down_back = swap(down_sent, "dp", dp, 1)
    g_up = dot(tokens, dpre_own, ((0,), (0,))) + up_back.astype(F32)
    g_down = dot(hid_own, d_tok, ((0,), (0,))) + down_back.astype(F32)
    grad_up = (
        lax.all_to_all(g_up.astype(BF16).reshape(dp, d_rows, f), "dp", 0, 0, tiled=True)
        .transpose(1, 0, 2)
        .reshape(d_rows, ff_m)
        .astype(F32)
    )
    grad_down = (
        lax.all_to_all(
            g_down.astype(BF16).reshape(f, dp, d_rows).transpose(1, 0, 2),
            "dp",
            0,
            0,
            tiled=True,
        )
        .reshape(ff_m, d_rows)
        .astype(F32)
    )

    block_out = (joined32 + gate * branch).astype(BF16)
    d_normed = d_mod * (1.0 + scale)
    d_full = d_out32 + inv_std * (
        d_normed
        - jnp.mean(d_normed, axis=-1, keepdims=True)
        - normed * jnp.mean(d_normed * normed, axis=-1, keepdims=True)
    )
    null_part = jnp.where(dropped, d_full[:n_text], F32(0.0)).astype(BF16)
    null_sum = lax.psum(null_part, "dp")

    def whole(rows):
        every = lax.all_gather(rows, "mp", axis=0)
        return jnp.concatenate(
            [
                every[:, :n_text].reshape(-1, width),
                every[:, n_text:].reshape(-1, width),
            ],
            axis=0,
        )[None]

    grad_null = lax.all_gather(null_sum, "mp", axis=0, tiled=True).astype(F32)
    return (whole(block_out), whole(d_full.astype(BF16)), grad_up, grad_down, grad_null)


class Place:
    def __init__(self, dp, mp):
        self.Z, self.X = dp // Y, mp // C
        d, m = lax.axis_index("dp"), lax.axis_index("mp")
        self.z, self.y = d // Y, d % Y
        self.x, self.c = m // C, m % C
        self.d, self.m = d, m

    def at_z(self, z):
        return (z * Y + self.y, self.m)

    def at_y(self):
        return (self.z * Y + 1 - self.y, self.m)

    def at_x(self, x):
        return (self.d, x * C + self.c)

    def at_c(self):
        return (self.d, self.x * C + 1 - self.c)

    def z_plus(self, j):
        return lax.rem(self.z + j, self.Z)

    def x_plus(self, j):
        return lax.rem(self.x + j, self.X)

    def meet(self):
        barrier = pltpu.get_barrier_semaphore()
        peers = [self.at_z(self.z_plus(j)) for j in range(1, self.Z)]
        peers += [self.at_x(self.x_plus(j)) for j in range(1, self.X)]
        peers += [self.at_y(), self.at_c()]
        for peer in peers:
            pl.semaphore_signal(barrier, inc=1, device_id=peer, device_id_type=MESH)
        pl.semaphore_wait(barrier, len(peers))


class Copies:
    def __init__(self, sems):
        self.sems, self.used, self.open = sems, 0, []

    def go(self, src, dst, recv, device, when=None):
        sem = self.sems.at[self.used]
        self.used += 1

        source, target, peer = src(), dst(), device()

        def make():
            return pltpu.make_async_remote_copy(
                src_ref=source,
                dst_ref=target,
                send_sem=sem,
                recv_sem=recv,
                device_id=peer,
                device_id_type=MESH,
            )

        def start():
            make().start()

        def finish():
            make().wait_send()

        guard(when, start)
        self.open.append((when, finish))

    def local(self, src, dst, when=None):
        sem = self.sems.at[self.used]
        self.used += 1

        source, target = src(), dst()

        def make():
            return pltpu.make_async_copy(source, target, sem)

        def start():
            make().start()

        def finish():
            make().wait()

        guard(when, start)
        self.open.append((when, finish))

    def finish(self):
        for when, wait in self.open:
            guard(when, wait)
        self.open = []


def guard(when, act):
    if when is None:
        act()
    else:
        pl.when(when)(act)


def landed(place, ref, recv, when=None):
    def act():
        pltpu.make_async_remote_copy(
            src_ref=ref(),
            dst_ref=ref(),
            send_sem=recv,
            recv_sem=recv,
            device_id=place.at_y(),
            device_id_type=MESH,
        ).wait_recv()

    guard(when, act)


def tile(index, size):
    return pl.ds(pl.multiple_of(index * size, size), size)


def add_into(target, other, rows, step):
    def body(i, _):
        at = pl.ds(pl.multiple_of(i * step, step), step)
        target[at, :] = (target[at, :].astype(F32) + other[at, :].astype(F32)).astype(BF16)
        return 0

    lax.fori_loop(0, rows // step, body, 0)


def each(first, last, act):
    def body(i, _):
        act(i)
        return 0

    lax.fori_loop(first, last, body, 0)


def block_kernel(
    dp,
    mp,
    nch,
    drop,
    level,
    image,
    text,
    null_prompt,
    d_output,
    w_up,
    w_down,
    out_all,
    d_tok_all,
    null_all,
    up_out,
    down_out,
    joined,
    text_v,
    null_v,
    d_out,
    tok,
    up,
    down,
    hid,
    d_pre,
    g_up,
    g_down,
    y_up,
    y_down,
    s_buf,
    c_buf,
    x_buf,
    l_buf,
    fin,
    null,
    null_y,
    null_z,
    send,
    z_tok,
    x_tok,
    c_tok,
    z_w,
    y_w,
    y_out,
    y_g,
    z_out,
    z_g,
    c_s,
    x_s,
    r_s,
    l_s,
    f_x,
    f_c,
    n_y,
    n_z,
    n_x,
    n_c,
    loads,
):
    p = Place(dp, mp)
    Z, X = p.Z, p.X
    dr = w_up.shape[0]
    fz = w_up.shape[1] // Z
    fch = fz // nch
    width = dr * dp
    n_text, n_image = text.shape[1] // mp, image.shape[1] // mp
    n = n_text + n_image
    half = Z * X * n
    rows = C * half
    cp = Copies(send)
    if Z == 4:
        one = jnp.where(p.z < 2, 1, 3)
        hops = [2, one, Z - one]
    else:
        hops = list(range(1, Z))

    def at_rows(c, z, x):
        return pl.ds(pl.multiple_of(((c * Z + z) * X + x) * n, n), n)

    every_text = text.shape[1]
    text_at = pl.ds(pl.multiple_of(p.m * n_text, n_text), n_text)
    image_at = pl.ds(pl.multiple_of(p.m * n_image, n_text), n_image)
    later = pl.ds(pl.multiple_of(every_text + p.m * n_image, n_text), n_image)
    first = [
        pltpu.make_async_copy(text.at[0, text_at], text_v, loads.at[0]),
        pltpu.make_async_copy(null_prompt.at[text_at], null_v, loads.at[1]),
        pltpu.make_async_copy(image.at[0, image_at], joined.at[pl.ds(n_text, n_image)], loads.at[2]),
        pltpu.make_async_copy(d_output.at[0, text_at], d_out.at[pl.ds(0, n_text)], loads.at[3]),
        pltpu.make_async_copy(d_output.at[0, later], d_out.at[pl.ds(n_text, n_image)], loads.at[4]),
    ]
    for copy in first:
        copy.start()
    p.meet()

    def up_src(z, k):
        return w_up.at[:, pl.ds(pl.multiple_of(z * fz + k * fch, fch), fch)]

    def down_src(z, k):
        return w_down.at[pl.ds(pl.multiple_of(z * fz + k * fch, fch), fch), :]

    def up_dst(d, k):
        return up.at[tile(d, dr), pl.ds(k * fch, fch)]

    def down_dst(d, k):
        return down.at[pl.ds(k * fch, fch), tile(d, dr)]

    kinds = ((up_src, up_dst), (down_src, down_dst))

    def z_weights(k, which):
        for j in which:
            for kind, (src, dst) in enumerate(kinds):
                cp.go(
                    lambda: src(p.z_plus(j), k),
                    lambda: dst(p.d, k),
                    z_w.at[j - 1, k, kind],
                    lambda: p.at_z(p.z_plus(j)),
                )

    def forward(k, j):
        d_src = lax.rem(p.z - j + Z, Z) * Y + p.y
        for kind, (_, dst) in enumerate(kinds):
            landed(p, lambda: dst(d_src, k), z_w.at[j - 1, k, kind])
            cp.go(lambda: dst(d_src, k), lambda: dst(d_src, k), y_w.at[j, k, kind], p.at_y)

    def weights_here(k):
        for j in range(Z):
            d_src = lax.rem(p.z - j + Z, Z) * Y + 1 - p.y
            for kind, (_, dst) in enumerate(kinds):
                landed(p, lambda: dst(d_src, k), y_w.at[j, k, kind])

    own_weights = []
    for k in range(nch):
        for kind, (src, dst) in enumerate(kinds):
            cp.go(lambda: src(p.z, k), lambda: dst(p.d, k), y_w.at[0, k, kind], p.at_y)
            copy = pltpu.make_async_copy(src(p.z, k), dst(p.d, k), loads.at[5 + 2 * k + kind])
            copy.start()
            own_weights.append(copy)

    for copy in first:
        copy.wait()
    joined[pl.ds(0, n_text)] = jnp.where(drop[0] == 1, null_v[...], text_v[...])
    shift, scale, gate = level[0:1, :], 1.0 + level[1:2, :], level[2:3, :]

    def stats(at):
        values = joined[at, :].astype(F32)
        centred = values - jnp.mean(values, axis=-1, keepdims=True)
        inv_std = lax.rsqrt(jnp.mean(centred * centred, axis=-1, keepdims=True) + EPS)
        return values, centred * inv_std, inv_std

    mine = pl.multiple_of(((p.c * Z + p.z) * X + p.x) * n, n)

    def prepare(b):
        at = pl.ds(pl.multiple_of(b * n_text, n_text), n_text)
        to = pl.ds(pl.multiple_of(mine + b * n_text, n_text), n_text)
        _, normed, _ = stats(at)
        tok[0, to, :] = (normed * scale + shift).astype(BF16)
        tok[1, to, :] = (d_out[at, :].astype(F32) * gate).astype(BF16)

    each(0, n // n_text, prepare)

    slots = [(0, p.z, None)]
    for s in range(Z - 1):
        slots.append((1 + 2 * s, p.z - 1 - s, p.z - 1 - s >= 0))
        slots.append((2 + 2 * s, p.z + 1 + s, p.z + 1 + s < Z))

    def block(sample, x, c):
        return tok.at[:, at_rows(c, sample, x), :]

    def spread(slot, sample, when):
        def ref():
            return block(sample, p.x, p.c)

        for j in range(1, X):
            cp.go(ref, ref, x_tok.at[j - 1, slot], lambda: p.at_x(p.x_plus(j)), when)
        cp.go(ref, ref, c_tok.at[0, slot], p.at_c, when)

    def pass_on(s, i):
        for way in (1, -1):
            sample = p.z - s * way
            inside = (sample >= 0) & (p.z + 1 < Z) if way == 1 else (sample < Z) & (p.z >= 1)

            def ref():
                return tok.at[i, at_rows(p.c, sample, p.x), :]

            cp.go(ref, ref, z_tok.at[(0 if way == 1 else 1), s, i], lambda: p.at_z(p.z + way), inside)

    for i in range(2):
        pass_on(0, i)
    spread(*slots[0])
    for s in range(Z - 1):
        for i in range(2):
            for side in (0, 1):
                slot, sample, valid = slots[1 + 2 * s + side]
                landed(p, lambda: tok.at[i, at_rows(p.c, sample, p.x), :], z_tok.at[side, s, i], valid)
            if s < Z - 2:
                pass_on(s + 1, i)
        for side in (0, 1):
            spread(*slots[1 + 2 * s + side])
        if s == min(1, Z - 2):
            z_weights(0, hops)
            forward(0, hops[0])
    forward(0, hops[1])
    z_weights(1, hops)
    for j in hops[2:]:
        forward(0, j)
    for slot, sample, valid in slots:
        for j in range(1, X):
            x = lax.rem(p.x - j + X, X)

            def ref():
                return block(sample, x, p.c)

            landed(p, ref, x_tok.at[j - 1, slot], valid)
            cp.go(ref, ref, c_tok.at[j, slot], p.at_c, valid)
    for k in range(2, nch):
        z_weights(k, hops)
    for slot, sample, valid in slots:
        for j in range(X):
            x = lax.rem(p.x - j + X, X)
            landed(p, lambda: block(sample, x, 1 - p.c), c_tok.at[j, slot], valid)

    tall = 256

    def hidden(k):
        units = pl.ds(k * fch, fch)

        def act(r):
            at = pl.ds(pl.multiple_of(r * tall, tall), tall)
            pre = dot(tok[0, at, :], up[:, units], ((1,), (0,)))
            d_hid = dot(tok[1, at, :], down[units, :], ((1,), (1,)))
            values, back = jax.vjp(gelu_tanh, pre)
            hid[at, units] = values.astype(BF16)
            d_pre[at, units] = back(d_hid)[0].astype(BF16)

        each(0, rows // tall, act)

    def y_copy(i, kind):
        k, j, z = place_of(i)
        ref = g_ref(kind, z, k)
        return pltpu.make_async_remote_copy(
            src_ref=ref((g_up, g_down)[kind]),
            dst_ref=ref((y_up, y_down)[kind]),
            send_sem=y_out.at[j, k, kind],
            recv_sem=y_g.at[j, k, kind],
            device_id=p.at_y(),
            device_id_type=MESH,
        )

    along = sorted(range(1, Z), key=lambda j: -min(j, Z - j))
    pieces = [(k, j) for j in along for k in range(nch - 1)]
    early = len(pieces)
    pieces += [(nch - 1, j) for j in along] + [(k, 0) for k in range(nch)]

    def place_of(i):
        k, j = pieces[i]
        return k, j, p.z_plus(j)

    def units_of(k):
        return pl.ds(k * fch, fch)

    def g_ref(kind, z, k):
        def ref(buffer):
            return buffer.at[tile(z, dr), units_of(k)] if kind == 0 else buffer.at[units_of(k), tile(z, dr)]

        return ref

    def product(kind, z, y, k):
        features = tile(z * Y + y, dr)
        if kind == 0:
            return dot(tok[0, :, features], d_pre[:, units_of(k)], ((0,), (0,)))
        return dot(hid[:, units_of(k)], tok[1, :, features], ((0,), (0,)))

    def peer_gradient(i):
        k, j, z = place_of(i)
        for kind in range(2):
            g_ref(kind, z, k)((g_up, g_down)[kind])[...] = product(kind, z, 1 - p.y, k).astype(BF16)
            y_copy(i, kind).start()

    def out_ref(kind, z, k):
        cols = pl.ds(pl.multiple_of(z * fz + k * fch, fch), fch)
        return up_out.at[:, cols] if kind == 0 else down_out.at[cols, :]

    def z_copy(i, kind):
        k, j, z = place_of(i)
        return pltpu.make_async_remote_copy(
            src_ref=g_ref(kind, z, k)((y_up, y_down)[kind]),
            dst_ref=out_ref(kind, p.z, k),
            send_sem=z_out.at[j, k, kind],
            recv_sem=z_g.at[j, k, kind],
            device_id=p.at_z(z),
            device_id_type=MESH,
        )

    def kept(i, kind):
        k, j, z = place_of(i)
        return pltpu.make_async_copy(
            g_ref(kind, z, k)((y_up, y_down)[kind]), out_ref(kind, p.z, k), z_out.at[j, k, kind]
        )

    def own_gradient(i):
        k, j, z = place_of(i)
        for kind in range(2):
            y_copy(i, kind).wait_recv()
            ref = g_ref(kind, z, k)((y_up, y_down)[kind])
            ref[...] = (product(kind, z, p.y, k) + ref[...].astype(F32)).astype(BF16)
            if j > 0:
                z_copy(i, kind).start()
            else:
                kept(i, kind).start()

    count = nch * Z
    started, ended = [0], [0]

    def some_peer(number):
        last = min(count, started[0] + number)
        if last > started[0]:
            for i in range(started[0], last):
                peer_gradient(i)
            started[0] = last

    def some_own(number):
        last = min(started[0], ended[0] + number)
        if last > ended[0]:
            for i in range(ended[0], last):
                own_gradient(i)
            ended[0] = last

    for copy in own_weights:
        copy.wait()
    weights_here(0)
    hidden(0)
    for j in hops:
        forward(1, j)
        if j is hops[1]:
            some_peer(1)
    for k in range(1, nch):
        if k + 1 < nch:
            for j in hops[:-1]:
                forward(k + 1, j)
        weights_here(k)
        hidden(k)
        if k + 1 < nch:
            forward(k + 1, hops[-1])
        if k == nch - 2:
            some_own(1)
            some_peer(early - started[0])

    wide = 256

    def summand(i, c, b):
        at = pl.ds(pl.multiple_of(c * half, half), half)
        cols = pl.ds(pl.multiple_of(b * wide, wide), wide)
        if i == 0:
            return cols, dot(hid[at, :], down[:, cols], ((1,), (0,)))
        return cols, dot(d_pre[at, :], up[cols, :], ((1,), (1,)))

    order = []
    for i in range((Z + 1) // 2):
        order += [Z - 1 - i] + ([i] if i != Z - 1 - i else [])

    def sample_rows(t):
        return pl.ds(t * X * n, X * n)

    def c_copy(i, t):
        return pltpu.make_async_remote_copy(
            src_ref=s_buf.at[i, sample_rows(t), :],
            dst_ref=c_buf.at[i, sample_rows(t), :],
            send_sem=c_s.at[0, i, t],
            recv_sem=c_s.at[1, i, t],
            device_id=p.at_c(),
            device_id_type=MESH,
        )

    def x_rows(t, x):
        return pl.ds(pl.multiple_of((t * X + x) * n, n), n)

    def own_rows(t):
        return x_rows(t, p.x)

    def other_core(i):
        def other(b):
            cols, value = summand(i, 1 - p.c, b)
            s_buf[i, :, cols] = value.astype(BF16)

        each(0, width // wide, other)
        for t in order:
            c_copy(i, t).start()

    def own_core(i):
        for t in order:
            c_copy(i, t).wait_recv()

        def mine_too(b):
            cols, value = summand(i, p.c, b)
            c_buf[i, :, cols] = (value + c_buf[i, :, cols].astype(F32)).astype(BF16)

        each(0, width // wide, mine_too)
        for t in order:
            for j in range(1, X):
                x = p.x_plus(j)
                cp.go(
                    lambda: c_buf.at[i, x_rows(t, x), :],
                    lambda: x_buf.at[j - 1, i, t],
                    x_s.at[j - 1, i, t],
                    lambda: p.at_x(x),
                )

    def x_stage(t, i):
        for j in range(X - 1):
            landed(p, lambda: x_buf.at[j, i, t], x_s.at[j, i, t])
            add_into(c_buf.at[i, own_rows(t), :], x_buf.at[j, i, t], n, 16)

    def chain(t, i, hop):
        for way, here_z, slot, sem in (
            (1, hop, t, r_s),
            (-1, Z - 1 - hop, t, l_s),
        ):
            if (t - here_z) * way <= 0:
                continue
            here = p.z == here_z
            target = Z if way == -1 and here_z - 1 == t else t
            if hop == 0:
                source = lambda: c_buf.at[i, own_rows(t), :]
            else:
                source = lambda: l_buf.at[i, t]
                landed(p, source, sem.at[i, t], here)
                pl.when(here)(lambda: add_into(l_buf.at[i, t], c_buf.at[i, own_rows(t), :], n, 16))
            cp.go(source, lambda: l_buf.at[i, target], sem.at[i, t], lambda: p.at_z(here_z + way), here)

    is_dropped = (drop[0] == 1).astype(F32)

    def arrived(i):
        for t in range(Z):
            here = p.z == t
            if t > 0:
                landed(p, lambda: l_buf.at[i, t], r_s.at[i, t], here)
            if t < Z - 1:
                landed(p, lambda: l_buf.at[i, Z], l_s.at[i, t], here)

    def total(i, b, at):
        mine_at = pl.ds(pl.multiple_of((p.z * X + p.x) * n + b * n_text, n_text), n_text)
        own = c_buf[i, mine_at, :].astype(F32)
        low = l_buf[i, p.z, at, :].astype(F32)
        high = l_buf[i, Z, at, :].astype(F32)
        return own + jnp.where(p.z > 0, low, 0.0) + jnp.where(p.z < Z - 1, high, 0.0)

    def output(b):
        at = pl.ds(pl.multiple_of(b * n_text, n_text), n_text)
        fin[0, at, :] = (joined[at, :].astype(F32) + gate * total(0, b, at)).astype(BF16)

    def input_gradient(b):
        at = pl.ds(pl.multiple_of(b * n_text, n_text), n_text)
        _, normed, inv_std = stats(at)
        d_normed = total(1, b, at) * scale
        d_full = d_out[at, :].astype(F32) + inv_std * (
            d_normed
            - jnp.mean(d_normed, axis=-1, keepdims=True)
            - normed * jnp.mean(d_normed * normed, axis=-1, keepdims=True)
        )
        fin[1, at, :] = d_full.astype(BF16)

        @pl.when(b == 0)
        def _():
            null[0] = (d_full * is_dropped).astype(BF16)

    def share(src, out, x_sem, c_sem):
        for j in range(1, X):
            cp.go(src, lambda: out(p.m), x_sem.at[j - 1], lambda: p.at_x(p.x_plus(j)))
        cp.go(src, lambda: out(p.m), c_sem.at[0], p.at_c)
        cp.local(src, lambda: out(p.m))

    def relay(out, x_sem, c_sem):
        for j in range(1, X):
            quarter = lax.rem(p.x - j + X, X) * C + p.c
            landed(p, lambda: out(quarter), x_sem.at[j - 1])
            cp.go(lambda: out(quarter), lambda: out(quarter), c_sem.at[j], p.at_c)

    def settle(out, c_sem):
        for j in range(X):
            quarter = lax.rem(p.x - j + X, X) * C + 1 - p.c
            landed(p, lambda: out(quarter), c_sem.at[j])

    def part(i, s):
        def out(quarter):
            if s == 0:
                at = pl.ds(pl.multiple_of(quarter * n_text, n_text), n_text)
            else:
                at = pl.ds(pl.multiple_of(every_text + quarter * n_image, n_text), n_image)
            return (out_all, d_tok_all)[i].at[at, :]

        return out

    def share_tokens(i):
        for s, at in enumerate((pl.ds(0, n_text), pl.ds(n_text, n_image))):
            share(lambda: fin.at[i, at, :], part(i, s), f_x.at[2 * i + s], f_c.at[2 * i + s])

    def relay_tokens(i):
        for s in range(2):
            relay(part(i, s), f_x.at[2 * i + s], f_c.at[2 * i + s])

    def null_out(quarter):
        return null_all.at[quarter]

    sums = [(t, i) for i in (1, 0) for t in order]
    lag = 3
    steps = len(sums) + lag * (Z - 2)

    def take(step):
        if step < len(sums):
            x_stage(*sums[step])
            chain(*sums[step], 0)
        if step < 3 or step in (len(sums) - 2, len(sums) + 1):
            some_own(1)
        for hop in range(Z - 2, 0, -1):
            at = step - hop * lag
            if 0 <= at < len(sums):
                chain(*sums[at], hop)
        if step == Z + lag * (Z - 2) + 1:
            arrived(1)
            each(0, n // n_text, input_gradient)
            cp.go(lambda: null.at[0], lambda: null_y.at[...], n_y.at[0], p.at_y)
            share_tokens(1)
            some_own(count)
            landed(p, lambda: null_y.at[...], n_y.at[0])
            null[1] = (null[0].astype(F32) + null_y[...].astype(F32)).astype(BF16)
            for j in range(1, Z):
                cp.go(lambda: null.at[1], lambda: null_z.at[j - 1], n_z.at[j - 1], lambda: p.at_z(p.z_plus(j)))

    some_own(1)
    some_peer(1)
    other_core(1)
    some_own(1)
    own_core(1)
    some_own(1)
    some_peer(2)
    other_core(0)
    take(0)
    own_core(0)
    some_peer(count)
    for step in range(1, steps):
        take(step)
    some_peer(count)
    some_own(count)
    relay_tokens(1)
    arrived(0)
    each(0, n // n_text, output)
    share_tokens(0)
    for j in range(1, Z):
        landed(p, lambda: null_z.at[j - 1], n_z.at[j - 1])
    whole_null = null[1].astype(F32)
    for j in range(1, Z):
        whole_null = whole_null + null_z[j - 1].astype(F32)
    null[2] = whole_null.astype(BF16)
    share(lambda: null.at[2], null_out, n_x, n_c)
    relay_tokens(0)
    relay(null_out, n_x, n_c)
    for i in range(2):
        for s in range(2):
            settle(part(i, s), f_c.at[2 * i + s])
    settle(null_out, n_c)

    def settled(i):
        k, j, z = place_of(i)
        for kind in range(2):
            y_copy(i, kind).wait_send()
            if j > 0:
                source = lax.rem(p.z - j + Z, Z)
                landed(p, lambda: out_ref(kind, source, k), z_g.at[j, k, kind])
                z_copy(i, kind).wait_send()
            else:
                kept(i, kind).wait()

    for i in range(count):
        settled(i)
    for i in range(2):
        for t in range(Z):
            c_copy(i, t).wait_send()
    cp.finish()


def shards(
    dp,
    mp,
    image_tokens,
    text_tokens,
    null_prompt,
    drop_flags,
    time_index,
    modulation,
    w_up,
    w_down,
    d_output,
):
    Z, X = dp // Y, mp // C
    d_rows, ff_m = w_up.shape
    fz = ff_m // Z
    nch = fz // 256
    width = d_rows * dp
    n_text = text_tokens.shape[1] // mp
    n = n_text + image_tokens.shape[1] // mp
    rows = Z * mp * n
    level = lax.dynamic_index_in_dim(modulation, time_index[0], 0, keepdims=False)

    anywhere = pl.BlockSpec(memory_space=pl.ANY)
    dma = pltpu.SemaphoreType.DMA
    slots = 1 + 2 * (Z - 1)
    sends = (
        2 * nch * Z
        + slots * (2 * X - 1)
        + 4 * (Z - 1)
        + 2 * nch * Z
        + 2 * Z * (X - 1)
        + 2 * 2 * Z * (Z - 1)
        + 1
        + (Z - 1)
        + 5 * (X + 1)
        + 5 * (X - 1)
    )
    every_out, every_d_tok, every_null, up_out, down_out = pl.pallas_call(
        functools.partial(block_kernel, dp, mp, nch),
        out_shape=(
            jax.ShapeDtypeStruct((mp * n, width), BF16),
            jax.ShapeDtypeStruct((mp * n, width), BF16),
            jax.ShapeDtypeStruct((mp, n_text, width), BF16),
            jax.ShapeDtypeStruct((d_rows, ff_m), BF16),
            jax.ShapeDtypeStruct((ff_m, d_rows), BF16),
        ),
        in_specs=[
            pl.BlockSpec(memory_space=pltpu.SMEM),
            pl.BlockSpec(memory_space=pltpu.VMEM),
        ]
        + [anywhere] * 6,
        out_specs=(anywhere,) * 5,
        scratch_shapes=[
            pltpu.VMEM((n, width), BF16),
            pltpu.VMEM((n_text, width), BF16),
            pltpu.VMEM((n_text, width), BF16),
            pltpu.VMEM((n, width), BF16),
            pltpu.VMEM((2, rows, width), BF16),
            pltpu.VMEM((width, fz), BF16),
            pltpu.VMEM((fz, width), BF16),
            pltpu.VMEM((rows, fz), BF16),
            pltpu.VMEM((rows, fz), BF16),
            pltpu.VMEM((Z * d_rows, fz), BF16),
            pltpu.VMEM((fz, Z * d_rows), BF16),
            pltpu.VMEM((Z * d_rows, fz), BF16),
            pltpu.VMEM((fz, Z * d_rows), BF16),
            pltpu.VMEM((2, rows // C, width), BF16),
            pltpu.VMEM((2, rows // C, width), BF16),
            pltpu.VMEM((X - 1, 2, Z, n, width), BF16),
            pltpu.VMEM((2, Z + 1, n, width), BF16),
            pltpu.VMEM((2, n, width), BF16),
            pltpu.VMEM((3, n_text, width), BF16),
            pltpu.VMEM((n_text, width), BF16),
            pltpu.VMEM((Z - 1, n_text, width), BF16),
            dma((sends,)),
            dma((2, Z - 1, 2)),
            dma((X - 1, slots)),
            dma((X, slots)),
            dma((Z - 1, nch, 2)),
            dma((Z, nch, 2)),
            dma((Z, nch, 2)),
            dma((Z, nch, 2)),
            dma((Z, nch, 2)),
            dma((Z, nch, 2)),
            dma((2, 2, Z)),
            dma((X - 1, 2, Z)),
            dma((2, Z)),
            dma((2, Z)),
            dma((4, X - 1)),
            dma((4, X)),
            dma((1,)),
            dma((Z - 1,)),
            dma((X - 1,)),
            dma((X,)),
            dma((5 + 2 * nch,)),
        ],
        compiler_params=pltpu.CompilerParams(
            collective_id=0, has_side_effects=True, vmem_limit_bytes=67043328
        ),
    )(drop_flags, level, image_tokens, text_tokens, null_prompt, d_output, w_up, w_down)

    return (
        every_out[None],
        every_d_tok[None],
        up_out.astype(F32),
        down_out.astype(F32),
        every_null.reshape(-1, width).astype(F32),
    )


def fits(dp, mp, image_tokens, text_tokens, w_up):
    d_rows, ff_m = w_up.shape
    return (
        dp % Y == 0
        and dp // Y > 2
        and mp % C == 0
        and mp // C > 1
        and d_rows % 128 == 0
        and ff_m % (dp // Y * 256) == 0
        and ff_m > dp // Y * 256
        and text_tokens.shape[1] % (mp * 16) == 0
        and image_tokens.shape[1] % text_tokens.shape[1] == 0
    )


def program(dp, mp, image_tokens, text_tokens, null_prompt, drop_flags, time_index, modulation, w_up, w_down, d_output):
    path = shards if fits(dp, mp, image_tokens, text_tokens, w_up) else generic
    return path(
        dp, mp, image_tokens, text_tokens, null_prompt, drop_flags, time_index, modulation, w_up, w_down, d_output
    )


def solution(mesh):
    placed = (
        P("dp", None, None),
        P("dp", None, None),
        P(),
        P("dp"),
        P("dp"),
        P(),
        P("dp", "mp"),
        P("mp", "dp"),
        P("dp", None, None),
    )
    return jax.shard_map(
        functools.partial(program, mesh.shape["dp"], mesh.shape["mp"]),
        mesh=mesh,
        in_specs=placed,
        out_specs=(P("dp", None, None), P("dp", None, None), P("dp", "mp"), P("mp", "dp"), P()),
        check_vma=False,
    )
```
